32 devices in a mesh: lat: 8 (over z, x), depth: 4 (over y, core).
Axes of the slice: x: 2, y: 2, z: 4, core: 2. Of those that a mesh axis runs over, the one named last changes fastest.
Arguments:
- surface: float32 [128, 4096], P('lat'), may hold values from -6 to 6
- velocity: float32 [2, 128, 4096], P(None, 'lat'), may hold values from -6 to 6
- block_map: int32 [128, 4096], P('lat'), may hold values from 0 to 15
- free_flags: int32 [128, 4096], P('lat'), may hold values 0 or 1
- block_rates: float32 [16], replicated, may hold values from 0.2 to 2
- previous_mesh: float32 [128, 64, 4096], P('lat', 'depth'), may hold values from -6 to 6
Outputs:
- new_surface: float32 [128, 4096], P('lat')
- mesh_field: float32 [128, 64, 4096], P('lat', 'depth')
- column_norm: float32 [128], P('lat')
The draws below stay inside these ranges and needn't reach their ends.
All inputs are finite; a program needn't handle non-finite values. No bound on the sum of `free_flags` on one device may be relied on, other than what follows from the above.
Results may differ from the reference program's by a relative error of at most 0.00002.
Values sent between devices are 32-bit elements; how exact they have to be, the bound alone decides.
A program may use at most 64 MiB of HBM per device.

```python
import math
import jax
import jax.numpy as jnp
from jax import lax

NY = 4096
NB = 16
ITERS = 2
NX = 128
NZ = 64


def touch_ends(result, key, least, top_value):
    place = [jax.random.randint(jax.random.fold_in(key, axis), (), 0, length) for axis, length in enumerate(result.shape)]
    main_axis = result.shape.index(max(result.shape))
    next_to = place[:main_axis] + [(place[main_axis] + 1) % result.shape[main_axis]] + place[main_axis + 1:]
    return result.at[tuple(place)].set(least).at[tuple(next_to)].set(top_value)


def shard_levels(stream_key, extent, cuts, low, largest):
    loudness = 1.0
    for position, parts in cuts:
        heights = jax.random.uniform(jax.random.fold_in(jax.random.fold_in(stream_key, 6), position), (parts,), jnp.float32, low / len(cuts), largest / len(cuts))
        loudness = loudness * jnp.repeat(jnp.exp(heights), extent[position] // parts).reshape((-1,) + (1,) * (len(extent) - 1 - position))
    return loudness


def bell_draw(key, extent, width, most, split=(), held_as=jnp.bfloat16):
    level = shard_levels(key, extent, split, -0.22, 0.18) if split else 1.0
    result = jax.random.normal(key, extent, jnp.float32) * width * level
    return jnp.minimum(jnp.maximum(result, -most), most).astype(held_as)


def setup_inputs(seed: int = 0) -> dict:
    keys = jax.random.split(jax.random.key(seed), 7)
    return {
        "surface": bell_draw(keys[0], (NX, NY), 1.0, 6.0, ((0, 8),), jnp.float32),
        "velocity": bell_draw(keys[1], (2, NX, NY), 1.0, 6.0, ((1, 8),), jnp.float32),
        "block_map": touch_ends(jax.random.randint(keys[2], (NX, NY), 0, NB), jax.random.fold_in(keys[2], 1), 0, NB - 1).astype(jnp.int32),
        "free_flags": touch_ends((jax.random.randint(keys[3], (NX, NY), 0, 4) < 3).astype(jnp.int32), jax.random.fold_in(keys[3], 1), 0, 1),
        "block_rates": jnp.clip(jnp.exp(jax.random.uniform(keys[4], (NB,), jnp.float32, math.log(0.2), math.log(2.0))), 0.2, 2.0),
        "previous_mesh": bell_draw(keys[5], (NX, NZ, NY), 1.0, 6.0, ((0, 8), (1, 4)), jnp.float32),
    }


TIME_STEP = 0.5
RELAX_WEIGHT = 0.8

def relax_once(field, surface_shift):
    padded_rows = jnp.pad(field, ((1, 1), (0, 0), (0, 0)))
    across_rows = padded_rows[2:] + padded_rows[:-2]
    padded_cols = jnp.pad(field, ((0, 0), (0, 0), (1, 1)))
    across_cols = padded_cols[:, :, 2:] + padded_cols[:, :, :-2]
    upper = jnp.concatenate([surface_shift[:, None, :], field[:, :-1, :]], axis=1)
    lower = jnp.concatenate([field[:, 1:, :], jnp.zeros_like(field[:, :1, :])], axis=1)
    neighbours = across_rows + across_cols + upper + lower
    return (1.0 - RELAX_WEIGHT) * field + RELAX_WEIGHT * neighbours / 6.0

def reference(surface, velocity, block_map, free_flags, block_rates, previous_mesh):
    padded = jnp.pad(surface, 1)
    grad_rows = (padded[2:, 1:-1] - padded[:-2, 1:-1]) * 0.5
    grad_cols = (padded[1:-1, 2:] - padded[1:-1, :-2]) * 0.5
    laplace = padded[2:, 1:-1] + padded[:-2, 1:-1] + padded[1:-1, 2:] + padded[1:-1, :-2] - 4.0 * surface
    diffusivity = block_rates[block_map]
    tendency = -velocity[0] * grad_rows - velocity[1] * grad_cols + diffusivity * laplace
    new_surface = surface + TIME_STEP * free_flags.astype(jnp.float32) * tendency
    surface_shift = new_surface - surface
    layers = jnp.arange(NZ, dtype=jnp.int32)
    profile = (NZ - layers).astype(jnp.float32) / NZ
    field = previous_mesh + surface_shift[:, None, :] * profile[None, :, None]
    for sweep_index in range(ITERS):
        field = relax_once(field, surface_shift)
    column_norm = jnp.sqrt(lax.optimization_barrier(jnp.sum(field * field, axis=(1, 2))) / (NZ * NY))
    return (new_surface, field, column_norm)
```

```python
import functools

import jax
import jax.numpy as jnp
from jax import lax
from jax.experimental import pallas as pl
from jax.experimental.pallas import tpu as pltpu
from jax.sharding import PartitionSpec as P

ITERS = 2
TIME_STEP = 0.5
RELAX_WEIGHT = 0.8
SIDE_WEIGHT = RELAX_WEIGHT / 6.0
MESH = pl.DeviceIdType.MESH
PAD = 128
TILE = 8
WIDTH = 512
CHUNKS = 4
RAW = 2
PARTNER, OUTER = 0, 1


def lanes_beside(window, width):
    span = window.shape[1]
    left = pltpu.roll(window, 1, 1)[:, PAD : PAD + width]
    right = pltpu.roll(window, span - 1, 1)[:, PAD : PAD + width]
    return window[:, PAD : PAD + width], left, right


def kernel(
    lats,
    depths,
    surface,
    velocity,
    block_map,
    free_flags,
    rates,
    previous,
    new_surface,
    field,
    norm,
    surf,
    vel,
    blocks,
    flags,
    shift,
    first,
    second,
    mine,
    theirs,
    relay,
    squares,
    sums,
    others,
    local_sem,
    near_send,
    near_recv,
    plane_send,
    plane_recv,
    relay_recv,
    forward_send,
    depth_send,
    depth_recv,
    sum_send,
    sum_recv,
):
    rows, layers, columns = previous.shape
    lat = lax.axis_index("lat")
    depth = lax.axis_index("depth")
    total_layers = layers * depths
    blocks_count = rates.shape[0]
    steps = columns // WIDTH
    piece = columns // CHUNKS
    per_piece = piece // WIDTH
    has_low, has_high = lat > 0, lat < lats - 1
    has_above, has_below = depth > 0, depth < depths - 1
    body_rows = pl.ds(TILE, rows)
    body_layers = pl.ds(TILE, layers)
    body_cols = pl.ds(PAD, columns)
    raw_cols = pl.ds(0, RAW * piece)

    odd = lax.rem(lat, 2)
    pair, pairs = lat // 2, lats // 2
    partner = lat + 1 - 2 * odd
    outward = lat - 1 + 2 * odd
    beyond = lat + 2 - 4 * odd
    behind = lat - 2 + 4 * odd
    has_outer = jnp.logical_and(outward >= 0, outward < lats)
    has_beyond = jnp.logical_and(beyond >= 0, beyond < lats)
    down_share = (2 * CHUNKS * pair) // pairs
    up_share = (2 * CHUNKS * (pairs - 1 - pair)) // pairs
    own_share = jnp.where(odd == 0, down_share, up_share)
    relay_share = jnp.where(odd == 0, up_share, down_share)
    low_side, high_side = odd, 1 - odd
    edges = (1 + (rows - 1) * high_side, 1 + (rows - 1) * low_side)
    inners = (2 + (rows - 3) * high_side, 2 + (rows - 3) * low_side)
    halos = ((rows + 1) * high_side, (rows + 1) * low_side)

    locals_ = [
        pltpu.make_async_copy(surface, surf.at[body_rows, body_cols], local_sem.at[0]),
        pltpu.make_async_copy(velocity, vel, local_sem.at[1]),
        pltpu.make_async_copy(block_map, blocks, local_sem.at[2]),
        pltpu.make_async_copy(free_flags, flags, local_sem.at[3]),
        pltpu.make_async_copy(
            previous, first.at[pl.ds(1, rows), body_layers, body_cols], local_sem.at[4]
        ),
    ]
    barrier = pltpu.get_barrier_semaphore()

    def greet(target):
        pl.semaphore_signal(barrier, inc=1, device_id=target, device_id_type=MESH)

    def lat_id(index):
        return {"lat": jnp.clip(index, 0, lats - 1)}

    greet(lat_id(partner))
    pl.when(has_outer)(lambda: greet(lat_id(outward)))
    pl.when(has_beyond)(lambda: greet(lat_id(beyond)))
    pl.when(has_outer)(lambda: greet(lat_id(behind)))
    for k in range(1, depths):
        greet({"depth": lax.rem(depth + k, depths)})
    for copy in locals_:
        copy.start()
    peers = depths + 2 * has_outer.astype(jnp.int32) + has_beyond.astype(jnp.int32)
    with jax.named_scope("p01_barrier"):
        pl.semaphore_wait(barrier, peers)

    def remote(src, dst, send, recv, target):
        return pltpu.make_async_remote_copy(
            src_ref=src,
            dst_ref=dst,
            send_sem=send,
            recv_sem=recv,
            device_id=target,
            device_id_type=MESH,
        )

    def nearby(side, slot, src, dst):
        target = lat_id(lat + 1 if side == 0 else lat - 1)
        return remote(src, dst, near_send.at[side, slot], near_recv.at[side, slot], target)

    def vertical(side, slot, src, dst):
        index = depth + 1 if side == 0 else depth - 1
        target = {"depth": jnp.clip(index, 0, depths - 1)}
        return remote(src, dst, depth_send.at[side, slot], depth_recv.at[side, slot], target)

    def piece_cols(k, pad=0):
        return pl.ds(pad + k * piece, piece)

    lat_sends = (has_high, has_low)
    lat_recvs = (has_low, has_high)
    depth_sends = (has_below, has_above)
    depth_recvs = (has_above, has_below)
    own_layer = (TILE + layers - 1, TILE)
    far_layer = (TILE - 1, TILE + layers)
    own_row = (TILE + rows - 1, TILE)
    far_row = (TILE - 1, TILE + rows)

    surf_copies = [
        nearby(
            side,
            0,
            surface.at[pl.ds((rows - 1, 0)[side], 1), :],
            surf.at[pl.ds(far_row[side], 1), body_cols],
        )
        for side in (0, 1)
    ]
    shift_copies = [
        nearby(
            side,
            1,
            shift.at[pl.ds(own_row[side], 1), raw_cols],
            shift.at[pl.ds(far_row[side], 1), raw_cols],
        )
        for side in (0, 1)
    ]

    def source(flow, c):
        if c < RAW:
            return previous.at[edges[flow] - 1, :, piece_cols(c)]
        if c < CHUNKS:
            return first.at[edges[flow], body_layers, piece_cols(c, PAD)]
        return mine.at[flow, :, piece_cols(c - CHUNKS)]

    def landing(flow, halo, c):
        if c < CHUNKS:
            return first.at[halo, body_layers, piece_cols(c, PAD)]
        return theirs.at[flow, :, piece_cols(c - CHUNKS)]

    partner_halo = (rows + 1) * low_side
    outward_halo = (rows + 1) * high_side
    beyond_halo = (rows + 1) * low_side
    planes = range(2 * CHUNKS)
    partner_copies = [
        remote(
            source(PARTNER, c),
            landing(PARTNER, partner_halo, c),
            plane_send.at[PARTNER, c],
            plane_recv.at[PARTNER, c],
            lat_id(partner),
        )
        for c in planes
    ]
    outward_copies = [
        remote(
            source(OUTER, c),
            landing(OUTER, outward_halo, c),
            plane_send.at[OUTER, c],
            plane_recv.at[OUTER, c],
            lat_id(outward),
        )
        for c in planes
    ]
    detour_copies = [
        remote(
            source(OUTER, c),
            relay.at[c],
            plane_send.at[OUTER, c],
            relay_recv.at[c],
            lat_id(partner),
        )
        for c in planes
    ]
    forward_copies = [
        remote(
            relay.at[c],
            landing(OUTER, beyond_halo, c),
            forward_send.at[c],
            plane_recv.at[OUTER, c],
            lat_id(beyond),
        )
        for c in planes
    ]

    def send_outer(c):
        pl.when(own_share > c)(detour_copies[c].start)
        pl.when(jnp.logical_and(has_outer, own_share <= c))(outward_copies[c].start)

    def forward(c):
        @pl.when(relay_share > c)
        def _():
            detour_copies[c].wait_recv()
            forward_copies[c].start()

    spans = (pl.ds(1, 1), pl.ds(rows, 1), pl.ds(2, rows - 2))
    raw_spans = (pl.ds(0, 1), pl.ds(rows - 1, 1), pl.ds(1, rows - 2))
    raw_layers = [
        [
            vertical(
                side,
                j,
                previous.at[raw, pl.ds((layers - 1, 0)[side], 1), :],
                first.at[span, pl.ds(far_layer[side], 1), body_cols],
            )
            for side in (0, 1)
        ]
        for j, (raw, span) in enumerate(zip(raw_spans, spans))
    ]
    later_layers = [
        [
            vertical(
                side,
                3 + j,
                second.at[span, pl.ds(own_layer[side], 1), body_cols],
                second.at[span, pl.ds(far_layer[side], 1), body_cols],
            )
            for side in (0, 1)
        ]
        for j, span in enumerate(spans)
    ]
    sum_copies = [
        remote(
            sums,
            others.at[k - 1],
            sum_send.at[k - 1],
            sum_recv.at[k - 1],
            {"depth": lax.rem(depth + k, depths)},
        )
        for k in range(1, depths)
    ]

    def start_layers(group):
        for side in (0, 1):
            pl.when(depth_sends[side])(group[side].start)

    def wait_layers(group):
        for side in (0, 1):
            pl.when(depth_recvs[side])(group[side].wait_recv)

    def send(c):
        send_outer(c)
        partner_copies[c].start()

    with jax.named_scope("p02_sends"):
        for side in (0, 1):
            pl.when(lat_sends[side])(surf_copies[side].start)
        send(0)
        for group in raw_layers[:2]:
            start_layers(group)
        send(1)
        start_layers(raw_layers[2])

    zero_tile = jnp.zeros((layers, PAD), jnp.float32)

    def clear_pads(r, carry):
        for buffer in (first, second):
            for start in (0, PAD + columns):
                buffer[r, body_layers, pl.ds(start, PAD)] = zero_tile
        return carry

    lax.fori_loop(1, rows + 1, clear_pads, 0)
    for start in (0, PAD + columns):
        surf[body_rows, pl.ds(start, PAD)] = jnp.zeros((rows, PAD), jnp.float32)
    squares[...] = jnp.zeros_like(squares)

    for side in (0, 1):

        @pl.when(jnp.logical_not(lat_recvs[side]))
        def _(side=side):
            surf[pl.ds(far_row[side], 1), body_cols] = jnp.zeros((1, columns), jnp.float32)
            shift[pl.ds(far_row[side], 1), :] = jnp.zeros((1, columns), jnp.float32)
            first[(0, rows + 1)[side], body_layers, body_cols] = jnp.zeros(
                (layers, columns), jnp.float32
            )
            theirs[OUTER] = jnp.zeros((layers, columns), jnp.float32)

    with jax.named_scope("p04_waitsurf"):
        for copy in locals_[:4]:
            copy.wait()
        for side in (0, 1):
            pl.when(lat_recvs[side])(surf_copies[side].wait_recv)

    def advect(step, carry):
        c = pl.multiple_of(step * WIDTH, WIDTH)
        cols = pl.ds(c, WIDTH)
        inner = pl.ds(pl.multiple_of(c + PAD, PAD), WIDTH)
        middle, left, right = lanes_beside(surf[body_rows, pl.ds(c, WIDTH + 2 * PAD)], WIDTH)
        before = pltpu.roll(surf[pl.ds(0, rows + TILE), inner], 1, 0)[TILE:]
        after = pltpu.roll(surf[pl.ds(TILE, rows + TILE), inner], rows + TILE - 1, 0)[:rows]
        grad_rows = (after - before) * 0.5
        grad_cols = (right - left) * 0.5
        laplace = after + before + right + left - 4.0 * middle
        names = blocks[:, cols]
        rate = jnp.full(names.shape, rates[0], jnp.float32)
        for label in range(1, blocks_count):
            rate = jnp.where(names == label, rates[label], rate)
        tendency = -vel[0, :, cols] * grad_rows - vel[1, :, cols] * grad_cols + rate * laplace
        fresh = middle + TIME_STEP * flags[:, cols].astype(jnp.float32) * tendency
        new_surface[:, cols] = fresh
        shift[body_rows, cols] = fresh - middle
        return carry

    with jax.named_scope("p05_advect"):
        lax.fori_loop(0, steps, advect, 0)
    with jax.named_scope("p06_sends"):
        for side in (0, 1):
            pl.when(lat_sends[side])(shift_copies[side].start)
        locals_[4].wait()

    def profile_of(index):
        return (total_layers - index).astype(jnp.float32) / total_layers

    base = depth * layers
    profile = profile_of(base + lax.broadcasted_iota(jnp.int32, (layers, PAD), 0))
    above_profile = profile_of(base - 1)
    below_profile = profile_of(base + layers)
    sublane = lax.broadcasted_iota(jnp.int32, (layers, WIDTH), 0)
    at_first = sublane == 0
    at_last = sublane == layers - 1
    above = pl.ds(TILE - 1, 1)
    below = pl.ds(TILE + layers, 1)

    def widen(r, c):
        inner = pl.ds(c + PAD, WIDTH)
        row_shift = jnp.broadcast_to(shift[pl.ds(TILE - 1 + r, 1), pl.ds(c, WIDTH)], (layers, WIDTH))
        wide_profile = jnp.concatenate([profile] * (WIDTH // PAD), axis=1)
        first[r, body_layers, inner] = first[r, body_layers, inner] + row_shift * wide_profile

    def in_plane(source, r, c, top, bottom):
        middle, left, right = lanes_beside(
            source[r, body_layers, pl.ds(c, WIDTH + 2 * PAD)], WIDTH
        )
        upper = jnp.where(at_first, top, pltpu.roll(middle, 1, 0))
        lower = jnp.where(at_last, bottom, pltpu.roll(middle, layers - 1, 0))
        return middle, (left + right) + (upper + lower)

    def first_ends(r, c):
        inner = pl.ds(c + PAD, WIDTH)
        row_shift = shift[pl.ds(TILE - 1 + r, 1), pl.ds(c, WIDTH)]
        top = jnp.where(has_above, first[r, above, inner] + row_shift * above_profile, row_shift)
        bottom = jnp.where(has_below, first[r, below, inner] + row_shift * below_profile, 0.0)
        return top, bottom

    def second_ends(r, c):
        inner = pl.ds(c + PAD, WIDTH)
        row_shift = shift[pl.ds(TILE - 1 + r, 1), pl.ds(c, WIDTH)]
        top = jnp.where(has_above, second[r, above, inner], row_shift)
        bottom = jnp.where(has_below, second[r, below, inner], 0.0)
        return top, bottom

    def weigh(middle, neighbours):
        return (1.0 - RELAX_WEIGHT) * middle + SIDE_WEIGHT * neighbours

    def partial(flow, c):
        inner = pl.ds(c + PAD, WIDTH)
        middle, around = in_plane(first, edges[flow], c, *first_ends(edges[flow], c))
        mine[flow, :, pl.ds(c, WIDTH)] = weigh(
            middle, around + first[inners[flow], body_layers, inner]
        )

    def complete(flow, c):
        inner = pl.ds(c + PAD, WIDTH)
        second[edges[flow], body_layers, inner] = (
            mine[flow, :, pl.ds(c, WIDTH)] + SIDE_WEIGHT * first[halos[flow], body_layers, inner]
        )

    def sweep_once(r, c):
        inner = pl.ds(c + PAD, WIDTH)
        middle, around = in_plane(first, r, c, *first_ends(r, c))
        across = first[r - 1, body_layers, inner] + first[r + 1, body_layers, inner]
        second[r, body_layers, inner] = weigh(middle, across + around)

    def tally(r, c, value):
        field[r - 1, :, pl.ds(c, WIDTH)] = value
        power = value * value
        part = squares[r - 1]
        for top in range(0, layers, TILE):
            for start in range(0, WIDTH, PAD):
                part = part + power[top : top + TILE, start : start + PAD]
        squares[r - 1] = part

    def sweep_twice(r, c):
        inner = pl.ds(c + PAD, WIDTH)
        middle, around = in_plane(second, r, c, *second_ends(r, c))
        across = second[r - 1, body_layers, inner] + second[r + 1, body_layers, inner]
        tally(r, c, weigh(middle, across + around))

    reach = (jnp.float32(SIDE_WEIGHT), jnp.where(has_outer, SIDE_WEIGHT, 0.0))

    def prepare(flow, c):
        inner = pl.ds(c + PAD, WIDTH)
        edge = edges[flow]
        middle, around = in_plane(second, edge, c, *second_ends(edge, c))
        around = around + second[inners[flow], body_layers, inner]
        facing_own = reach[flow] * first[edge, body_layers, inner]
        field[edge - 1, :, pl.ds(c, WIDTH)] = weigh(middle, around + facing_own)

    def finish(flow, c):
        cols = pl.ds(c, WIDTH)
        edge = edges[flow]
        tally(edge, c, field[edge - 1, :, cols] + SIDE_WEIGHT * theirs[flow, :, cols])

    def over(low, count, visit):
        def body(t, carry):
            for step in range(steps):
                visit(t, step * WIDTH)
            return carry

        lax.fori_loop(low, low + count, body, 0)

    with jax.named_scope("p07_widen"):
        over(1, 2, widen)
        over(rows - 1, 2, widen)
        send(2)
        send(3)
    with jax.named_scope("p08_waitraw"):
        for group in raw_layers[:2]:
            wait_layers(group)
    with jax.named_scope("p09_partial"):
        for flow in (OUTER, PARTNER):
            for step in range(steps):
                partial(flow, step * WIDTH)
    with jax.named_scope("p10_fwd0"):
        forward(0)
    with jax.named_scope("p11_widen"):
        over(3, rows - 4, widen)
        send(4)
    with jax.named_scope("p12_waitraw"):
        wait_layers(raw_layers[2])
    middle_row = rows // 2 + 1
    with jax.named_scope("p13_sweep1"):
        over(2, middle_row - 2, sweep_once)
    with jax.named_scope("p14_fwd1"):
        send(5)
        forward(1)
    with jax.named_scope("p15_sweep1"):
        over(middle_row, rows - middle_row, sweep_once)
        start_layers(later_layers[2])
    with jax.named_scope("p16_fwd2"):
        send(6)
        send(7)
        forward(2)
    with jax.named_scope("p17_waitshift"):
        for side in (0, 1):
            pl.when(lat_recvs[side])(shift_copies[side].wait_recv)
    for k in range(CHUNKS):
        if k == CHUNKS - 1:
            with jax.named_scope("p18_fwd3"):
                forward(3)
        for flow in (PARTNER, OUTER):

            def arrive(flow=flow, k=k):
                (partner_copies, outward_copies)[flow][k].wait_recv()
                for j in range(per_piece if k < RAW else 0):
                    widen(halos[flow], k * piece + j * WIDTH)

            with jax.named_scope(f"p18_{k}{'po'[flow]}"):
                if flow == PARTNER:
                    arrive()
                else:
                    pl.when(has_outer)(arrive)
            for j in range(per_piece):
                complete(flow, k * piece + j * WIDTH)
    with jax.named_scope("p19_edges"):
        for j in (0, 1):
            start_layers(later_layers[j])
    with jax.named_scope("p20_waitlater"):
        wait_layers(later_layers[2])
    with jax.named_scope("p22_sweep2"):
        over(2, rows - 2, sweep_twice)
    with jax.named_scope("p23_waitlater"):
        for j in (0, 1):
            wait_layers(later_layers[j])
    with jax.named_scope("p24_prepare"):
        for flow in (PARTNER, OUTER):
            for step in range(steps):
                prepare(flow, step * WIDTH)

    for k in range(CHUNKS):
        with jax.named_scope(f"p25_finish{k}"):
            forward(CHUNKS + k)
            for flow in (PARTNER, OUTER):
                if flow == PARTNER:
                    partner_copies[CHUNKS + k].wait_recv()
                else:
                    pl.when(has_outer)(outward_copies[CHUNKS + k].wait_recv)
                for j in range(per_piece):
                    finish(flow, k * piece + j * WIDTH)

    sums[...] = jnp.sum(squares[...], axis=1)
    for copy in sum_copies:
        copy.start()
    for side in (0, 1):
        for copy in (surf_copies[side], shift_copies[side]):
            pl.when(lat_sends[side])(copy.wait_send)
        for group in raw_layers + later_layers:
            pl.when(depth_sends[side])(group[side].wait_send)
    for c in planes:
        partner_copies[c].wait_send()
        pl.when(has_outer)(outward_copies[c].wait_send)
        pl.when(relay_share > c)(forward_copies[c].wait_send)
    with jax.named_scope("p27_waitsums"):
        for copy in sum_copies:
            copy.wait_recv()
        for copy in sum_copies:
            copy.wait_send()
    with jax.named_scope("p28_total"):
        total = sums[...]
        for k in range(depths - 1):
            total = total + others[k]
        norm[...] = total


def deliver(count, surface_in, field_in, total, surface_out, field_out, norm_out, packed, sem):
    copies = [
        pltpu.make_async_copy(field_in, field_out, sem.at[0]),
        pltpu.make_async_copy(surface_in, surface_out, sem.at[1]),
        pltpu.make_async_copy(packed, norm_out, sem.at[2]),
    ]
    for copy in copies[:2]:
        copy.start()
    rows, lanes = total.shape[0], pl.cdiv(total.shape[0], PAD) * PAD
    column = jnp.broadcast_to(jnp.sum(total[...], axis=1, keepdims=True), (rows, lanes))
    ids = lax.broadcasted_iota(jnp.int32, column.shape, 0)
    places = lax.broadcasted_iota(jnp.int32, column.shape, 1)
    flat = jnp.sum(jnp.where(ids == places, column, 0.0), axis=0, keepdims=True)
    packed[...] = jnp.sqrt(flat / count)[0, :rows]
    copies[2].start()
    for copy in copies:
        copy.wait()


def solution(mesh):
    lats, depths = mesh.shape["lat"], mesh.shape["depth"]

    def per_device(surface, velocity, block_map, free_flags, block_rates, previous_mesh):
        rows, layers, columns = previous_mesh.shape
        wide = columns + 2 * PAD
        anywhere = pl.BlockSpec(memory_space=pltpu.HBM)
        f32 = jnp.float32
        others = max(depths - 1, 1)
        dma = pltpu.SemaphoreType.DMA
        held = [
            pltpu.with_memory_space_constraint(value, pltpu.HBM)
            for value in (surface, velocity, block_map, free_flags, previous_mesh)
        ]
        results = pl.pallas_call(
            functools.partial(kernel, lats, depths),
            out_shape=(
                pltpu.VMEM(surface.shape, f32),
                pltpu.VMEM(previous_mesh.shape, f32),
                pltpu.VMEM((rows, PAD), f32),
            ),
            in_specs=[anywhere] * 4 + [pl.BlockSpec(memory_space=pltpu.SMEM), anywhere],
            out_specs=(pl.BlockSpec(memory_space=pltpu.VMEM),) * 3,
            scratch_shapes=[
                pltpu.VMEM((rows + 2 * TILE, wide), f32),
                pltpu.VMEM(velocity.shape, f32),
                pltpu.VMEM(block_map.shape, jnp.int32),
                pltpu.VMEM(free_flags.shape, jnp.int32),
                pltpu.VMEM((rows + 2 * TILE, columns), f32),
                pltpu.VMEM((rows + 2, layers + 2 * TILE, wide), f32),
                pltpu.VMEM((rows + 2, layers + 2 * TILE, wide), f32),
                pltpu.VMEM((2, layers, columns), f32),
                pltpu.VMEM((2, layers, columns), f32),
                pltpu.VMEM((2 * CHUNKS, layers, columns // CHUNKS), f32),
                pltpu.VMEM((rows, TILE, PAD), f32),
                pltpu.VMEM((rows, PAD), f32),
                pltpu.VMEM((others, rows, PAD), f32),
                dma((5,)),
                dma((2, 2)),
                dma((2, 2)),
                dma((2, 2 * CHUNKS)),
                dma((2, 2 * CHUNKS)),
                dma((2 * CHUNKS,)),
                dma((2 * CHUNKS,)),
                dma((2, 6)),
                dma((2, 6)),
                dma((others,)),
                dma((others,)),
            ],
            compiler_params=pltpu.CompilerParams(
                collective_id=0, has_side_effects=True, vmem_limit_bytes=56 * 1024 * 1024
            ),
            name="advect_and_relax",
        )(*held[:4], block_rates, held[4])
        resident = [pltpu.with_memory_space_constraint(value, pltpu.VMEM) for value in results]
        new_surface, field, norm = pl.pallas_call(
            functools.partial(deliver, layers * depths * columns),
            out_shape=(
                pltpu.HBM(surface.shape, f32),
                pltpu.HBM(previous_mesh.shape, f32),
                pltpu.HBM((rows,), f32),
            ),
            in_specs=[pl.BlockSpec(memory_space=pltpu.VMEM)] * 3,
            out_specs=(anywhere,) * 3,
            scratch_shapes=[pltpu.VMEM((rows,), f32), dma((3,))],
            compiler_params=pltpu.CompilerParams(vmem_limit_bytes=1024 * 1024),
            name="deliver",
        )(*resident)
        return new_surface, field, norm

    return jax.shard_map(
        per_device,
        mesh=mesh,
        in_specs=(
            P("lat", None),
            P(None, "lat", None),
            P("lat", None),
            P("lat", None),
            P(),
            P("lat", "depth", None),
        ),
        out_specs=(P("lat", None), P("lat", "depth", None), P("lat")),
        check_vma=False,
    )
```

```python
import functools

import jax
import jax.numpy as jnp
from jax import lax
from jax.experimental import pallas as pl
from jax.experimental.pallas import tpu as pltpu
from jax.sharding import PartitionSpec as P

ITERS = 2
TIME_STEP = 0.5
RELAX_WEIGHT = 0.8
SIDE_WEIGHT = RELAX_WEIGHT / 6.0
MESH = pl.DeviceIdType.MESH
PAD = 128
TILE = 8
WIDTH = 1024
CHUNKS = 4
RAW = (2, CHUNKS)
PARTNER, OUTER = 0, 1


def lanes_beside(window, width):
    span = window.shape[1]
    left = pltpu.roll(window, 1, 1)[:, PAD : PAD + width]
    right = pltpu.roll(window, span - 1, 1)[:, PAD : PAD + width]
    return window[:, PAD : PAD + width], left, right


def kernel(
    lats,
    depths,
    surface,
    velocity,
    block_map,
    free_flags,
    rates,
    previous,
    new_surface,
    field,
    norm,
    surf,
    vel,
    blocks,
    flags,
    shift,
    first,
    second,
    mine,
    theirs,
    relay,
    relay_shift,
    squares,
    sums,
    others,
    local_sem,
    near_send,
    near_recv,
    shift_send,
    shift_recv,
    plane_send,
    plane_recv,
    relay_recv,
    forward_send,
    depth_send,
    depth_recv,
    sum_send,
    sum_recv,
):
    rows, layers, columns = previous.shape
    lat = lax.axis_index("lat")
    depth = lax.axis_index("depth")
    total_layers = layers * depths
    blocks_count = rates.shape[0]
    steps = columns // WIDTH
    piece = columns // CHUNKS
    per_piece = piece // WIDTH
    has_low, has_high = lat > 0, lat < lats - 1
    has_above, has_below = depth > 0, depth < depths - 1
    body_rows = pl.ds(TILE, rows)
    body_layers = pl.ds(TILE, layers)
    body_cols = pl.ds(PAD, columns)

    odd = lax.rem(lat, 2)
    pair, pairs = lat // 2, lats // 2
    partner = lat + 1 - 2 * odd
    outward = lat - 1 + 2 * odd
    beyond = lat + 2 - 4 * odd
    behind = lat - 2 + 4 * odd
    has_outer = jnp.logical_and(outward >= 0, outward < lats)
    has_beyond = jnp.logical_and(beyond >= 0, beyond < lats)
    down_share = (2 * CHUNKS * pair) // pairs
    up_share = (2 * CHUNKS * (pairs - 1 - pair)) // pairs
    own_share = jnp.where(odd == 0, down_share, up_share)
    relay_share = jnp.where(odd == 0, up_share, down_share)
    low_side, high_side = odd, 1 - odd
    edges = (1 + (rows - 1) * high_side, 1 + (rows - 1) * low_side)
    inners = (2 + (rows - 3) * high_side, 2 + (rows - 3) * low_side)
    halos = ((rows + 1) * high_side, (rows + 1) * low_side)

    local_surface = pltpu.make_async_copy(
        surface, surf.at[body_rows, body_cols], local_sem.at[0]
    )
    local_inputs = [
        pltpu.make_async_copy(velocity, vel, local_sem.at[1]),
        pltpu.make_async_copy(block_map, blocks, local_sem.at[2]),
        pltpu.make_async_copy(free_flags, flags, local_sem.at[3]),
    ]
    local_mesh = pltpu.make_async_copy(
        previous, first.at[pl.ds(1, rows), body_layers, body_cols], local_sem.at[4]
    )

    barrier = pltpu.get_barrier_semaphore()

    def greet(target):
        pl.semaphore_signal(barrier, inc=1, device_id=target, device_id_type=MESH)

    def lat_id(index):
        return {"lat": jnp.clip(index, 0, lats - 1)}

    greet(lat_id(partner))
    pl.when(has_outer)(lambda: greet(lat_id(outward)))
    pl.when(has_beyond)(lambda: greet(lat_id(beyond)))
    pl.when(has_outer)(lambda: greet(lat_id(behind)))
    for k in range(1, depths):
        greet({"depth": lax.rem(depth + k, depths)})
    for copy in [local_surface, *local_inputs, local_mesh]:
        copy.start()
    peers = depths + 2 * has_outer.astype(jnp.int32) + has_beyond.astype(jnp.int32)
    with jax.named_scope("p01_barrier"):
        pl.semaphore_wait(barrier, peers)

    def remote(src, dst, send, recv, target):
        return pltpu.make_async_remote_copy(
            src_ref=src,
            dst_ref=dst,
            send_sem=send,
            recv_sem=recv,
            device_id=target,
            device_id_type=MESH,
        )

    def nearby(side, src, dst):
        target = lat_id(lat + 1 if side == 0 else lat - 1)
        return remote(src, dst, near_send.at[side], near_recv.at[side], target)

    def vertical(side, slot, src, dst):
        index = depth + 1 if side == 0 else depth - 1
        target = {"depth": jnp.clip(index, 0, depths - 1)}
        return remote(src, dst, depth_send.at[side], depth_recv.at[side, slot], target)

    def piece_cols(k, pad=0):
        return pl.ds(pad + k * piece, piece)

    lat_sends = (has_high, has_low)
    lat_recvs = (has_low, has_high)
    depth_sends = (has_below, has_above)
    depth_recvs = (has_above, has_below)
    own_layer = (TILE + layers - 1, TILE)
    far_layer = (TILE - 1, TILE + layers)
    own_row = (TILE + rows - 1, TILE)
    far_row = (TILE - 1, TILE + rows)

    surf_copies = [
        nearby(
            side,
            surf.at[pl.ds(own_row[side], 1), body_cols],
            surf.at[pl.ds(far_row[side], 1), body_cols],
        )
        for side in (0, 1)
    ]

    def shift_row(row, flow):
        return shift.at[pl.ds(row, 1), pl.ds(0, RAW[flow] * piece)]

    shift_partner = [
        remote(
            shift_row(own_row[side], PARTNER),
            shift_row(far_row[side], PARTNER),
            shift_send.at[0],
            shift_recv.at[0],
            lat_id(partner),
        )
        for side in (0, 1)
    ]
    shift_detour = [
        remote(
            shift_row(own_row[side], OUTER),
            relay_shift,
            shift_send.at[1],
            shift_recv.at[1],
            lat_id(partner),
        )
        for side in (0, 1)
    ]
    shift_forward = [
        remote(
            relay_shift,
            shift_row(far_row[side], OUTER),
            shift_send.at[2],
            shift_recv.at[2],
            lat_id(beyond),
        )
        for side in (0, 1)
    ]

    def send_shift():
        for side in (0, 1):
            toward = (odd == 0) if side == 0 else (odd == 1)
            away = jnp.logical_and(has_outer, (odd == 1) if side == 0 else (odd == 0))
            pl.when(away)(shift_detour[side].start)
            pl.when(toward)(shift_partner[side].start)

    def forward_shift():
        shift_detour[0].wait_recv()
        for side in (0, 1):
            pl.when((odd == 0) if side == 0 else (odd == 1))(shift_forward[side].start)

    def source(flow, c):
        if c < RAW[flow]:
            return previous.at[edges[flow] - 1, :, piece_cols(c)]
        if c < CHUNKS:
            return first.at[edges[flow], body_layers, piece_cols(c, PAD)]
        return mine.at[flow, :, piece_cols(c - CHUNKS)]

    def landing(flow, halo, c):
        if c < CHUNKS:
            return first.at[halo, body_layers, piece_cols(c, PAD)]
        return theirs.at[flow, :, piece_cols(c - CHUNKS)]

    partner_halo = (rows + 1) * low_side
    outward_halo = (rows + 1) * high_side
    beyond_halo = (rows + 1) * low_side
    pieces = range(2 * CHUNKS)
    order = list(pieces)
    most = (2 * CHUNKS * (pairs - 1)) // pairs
    detours = order[:most]

    def landed(flow, c):
        return plane_recv.at[flow, max(c - CHUNKS + 1, 0)]

    partner_copies = [
        remote(
            source(PARTNER, c),
            landing(PARTNER, partner_halo, c),
            plane_send.at[PARTNER],
            landed(PARTNER, c),
            lat_id(partner),
        )
        for c in pieces
    ]
    outward_copies = [
        remote(
            source(OUTER, c),
            landing(OUTER, outward_halo, c),
            plane_send.at[OUTER],
            landed(OUTER, c),
            lat_id(outward),
        )
        for c in pieces
    ]
    detour_copies = {
        c: remote(
            source(OUTER, c),
            relay.at[slot],
            plane_send.at[OUTER],
            relay_recv.at[slot],
            lat_id(partner),
        )
        for slot, c in enumerate(detours)
    }
    forward_copies = {
        c: remote(
            relay.at[slot],
            landing(OUTER, beyond_halo, c),
            forward_send.at[0],
            landed(OUTER, c),
            lat_id(beyond),
        )
        for slot, c in enumerate(detours)
    }

    def whole_plane(flow):
        whole = first.at[halos[flow], body_layers, body_cols]
        return remote(whole, whole, plane_send.at[flow], plane_recv.at[flow, 0], lat_id(partner))

    def send_detour(c):
        if c in detour_copies:
            pl.when(own_share > detours.index(c))(detour_copies[c].start)

    def send_direct(c):
        direct = has_outer
        if c in detour_copies:
            direct = jnp.logical_and(has_outer, own_share <= detours.index(c))
        pl.when(direct)(outward_copies[c].start)

    def forward(c):
        if c not in forward_copies:
            return

        @pl.when(relay_share > detours.index(c))
        def _():
            detour_copies[c].wait_recv()
            forward_copies[c].start()

    spans = (pl.ds(1, 1), pl.ds(rows, 1), pl.ds(2, rows - 2))
    raw_spans = (pl.ds(0, 1), pl.ds(rows - 1, 1), pl.ds(1, rows - 2))
    raw_layers = [
        [
            vertical(
                side,
                min(j, 2) // 2,
                previous.at[raw, pl.ds((layers - 1, 0)[side], 1), :],
                first.at[span, pl.ds(far_layer[side], 1), body_cols],
            )
            for side in (0, 1)
        ]
        for j, (raw, span) in enumerate(zip(raw_spans, spans))
    ]
    later_layers = [
        [
            vertical(
                side,
                2 + min(j, 2) // 2,
                second.at[span, pl.ds(own_layer[side], 1), body_cols],
                second.at[span, pl.ds(far_layer[side], 1), body_cols],
            )
            for side in (0, 1)
        ]
        for j, span in enumerate(spans)
    ]

    def edge_layers(buffer, slot):
        pair_span = pl.ds(1, 2)
        return [
            vertical(side, slot, *[buffer.at[pair_span, pl.ds(far_layer[side], 1), body_cols]] * 2)
            for side in (0, 1)
        ]

    sum_copies = [
        remote(
            sums,
            others.at[k - 1],
            sum_send.at[0],
            sum_recv.at[0],
            {"depth": lax.rem(depth + k, depths)},
        )
        for k in range(1, depths)
    ]

    def start_layers(group):
        for side in (0, 1):
            pl.when(depth_sends[side])(group[side].start)

    def wait_layers(group):
        for side in (0, 1):
            pl.when(depth_recvs[side])(group[side].wait_recv)

    with jax.named_scope("p02_sends"):
        local_surface.wait()
        for side in (0, 1):
            pl.when(lat_sends[side])(surf_copies[side].start)
        for group in raw_layers[:2]:
            start_layers(group)
        for c in range(RAW[OUTER]):
            send_detour(c)
        for c in range(RAW[PARTNER]):
            partner_copies[c].start()
        for c in range(RAW[OUTER]):
            send_direct(c)
        start_layers(raw_layers[2])

    zero_tile = jnp.zeros((layers, PAD), jnp.float32)

    def clear_pads(r, carry):
        for buffer in (first, second):
            for start in (0, PAD + columns):
                buffer[r, body_layers, pl.ds(start, PAD)] = zero_tile
        return carry

    lax.fori_loop(1, rows + 1, clear_pads, 0)
    for start in (0, PAD + columns):
        surf[body_rows, pl.ds(start, PAD)] = jnp.zeros((rows, PAD), jnp.float32)
    squares[...] = jnp.zeros_like(squares)

    for side in (0, 1):

        @pl.when(jnp.logical_not(lat_recvs[side]))
        def _(side=side):
            surf[pl.ds(far_row[side], 1), body_cols] = jnp.zeros((1, columns), jnp.float32)
            shift[pl.ds(far_row[side], 1), :] = jnp.zeros((1, columns), jnp.float32)
            first[(0, rows + 1)[side], body_layers, body_cols] = jnp.zeros(
                (layers, columns), jnp.float32
            )
            theirs[OUTER] = jnp.zeros((layers, columns), jnp.float32)

    with jax.named_scope("p04_waitsurf"):
        for copy in local_inputs:
            copy.wait()
        for side in (0, 1):
            pl.when(lat_recvs[side])(surf_copies[side].wait_recv)

    def advect(step, carry):
        c = pl.multiple_of(step * WIDTH, WIDTH)
        cols = pl.ds(c, WIDTH)
        inner = pl.ds(pl.multiple_of(c + PAD, PAD), WIDTH)
        middle, left, right = lanes_beside(surf[body_rows, pl.ds(c, WIDTH + 2 * PAD)], WIDTH)
        before = pltpu.roll(surf[pl.ds(0, rows + TILE), inner], 1, 0)[TILE:]
        after = pltpu.roll(surf[pl.ds(TILE, rows + TILE), inner], rows + TILE - 1, 0)[:rows]
        grad_rows = (after - before) * 0.5
        grad_cols = (right - left) * 0.5
        laplace = after + before + right + left - 4.0 * middle
        names = blocks[:, cols]
        rate = jnp.full(names.shape, rates[0], jnp.float32)
        for label in range(1, blocks_count):
            rate = jnp.where(names == label, rates[label], rate)
        tendency = -vel[0, :, cols] * grad_rows - vel[1, :, cols] * grad_cols + rate * laplace
        fresh = middle + TIME_STEP * flags[:, cols].astype(jnp.float32) * tendency
        new_surface[:, cols] = fresh
        shift[body_rows, cols] = fresh - middle
        return carry

    with jax.named_scope("p05_advect"):
        lax.fori_loop(0, steps, advect, 0)
    with jax.named_scope("p06_sends"):
        send_shift()
        local_mesh.wait()

    def profile_of(index):
        return (total_layers - index).astype(jnp.float32) / total_layers

    base = depth * layers
    profile = profile_of(base + lax.broadcasted_iota(jnp.int32, (layers, PAD), 0))
    above_profile = profile_of(base - 1)
    below_profile = profile_of(base + layers)
    sublane = lax.broadcasted_iota(jnp.int32, (layers, WIDTH), 0)
    at_first = sublane == 0
    at_last = sublane == layers - 1
    above = pl.ds(TILE - 1, 1)
    below = pl.ds(TILE + layers, 1)

    def widen(r, c):
        inner = pl.ds(c + PAD, WIDTH)
        row_shift = jnp.broadcast_to(shift[pl.ds(TILE - 1 + r, 1), pl.ds(c, WIDTH)], (layers, WIDTH))
        wide_profile = jnp.concatenate([profile] * (WIDTH // PAD), axis=1)
        first[r, body_layers, inner] = first[r, body_layers, inner] + row_shift * wide_profile

    def in_plane(source, r, c, top, bottom):
        middle, left, right = lanes_beside(
            source[r, body_layers, pl.ds(c, WIDTH + 2 * PAD)], WIDTH
        )
        upper = jnp.where(at_first, top, pltpu.roll(middle, 1, 0))
        lower = jnp.where(at_last, bottom, pltpu.roll(middle, layers - 1, 0))
        return middle, (left + right) + (upper + lower)

    def first_ends(r, c):
        inner = pl.ds(c + PAD, WIDTH)
        row_shift = shift[pl.ds(TILE - 1 + r, 1), pl.ds(c, WIDTH)]
        top = jnp.where(has_above, first[r, above, inner] + row_shift * above_profile, row_shift)
        bottom = jnp.where(has_below, first[r, below, inner] + row_shift * below_profile, 0.0)
        return top, bottom

    def second_ends(r, c):
        inner = pl.ds(c + PAD, WIDTH)
        row_shift = shift[pl.ds(TILE - 1 + r, 1), pl.ds(c, WIDTH)]
        top = jnp.where(has_above, second[r, above, inner], row_shift)
        bottom = jnp.where(has_below, second[r, below, inner], 0.0)
        return top, bottom

    def weigh(middle, neighbours):
        return (1.0 - RELAX_WEIGHT) * middle + SIDE_WEIGHT * neighbours

    def partial(flow, c):
        inner = pl.ds(c + PAD, WIDTH)
        middle, around = in_plane(first, edges[flow], c, *first_ends(edges[flow], c))
        mine[flow, :, pl.ds(c, WIDTH)] = weigh(
            middle, around + first[inners[flow], body_layers, inner]
        )

    def complete(flow, c):
        inner = pl.ds(c + PAD, WIDTH)
        second[edges[flow], body_layers, inner] = (
            mine[flow, :, pl.ds(c, WIDTH)] + SIDE_WEIGHT * first[halos[flow], body_layers, inner]
        )

    def sweep_once(r, c):
        inner = pl.ds(c + PAD, WIDTH)
        middle, around = in_plane(first, r, c, *first_ends(r, c))
        across = first[r - 1, body_layers, inner] + first[r + 1, body_layers, inner]
        second[r, body_layers, inner] = weigh(middle, across + around)

    def tally(r, c, value):
        field[r - 1, :, pl.ds(c, WIDTH)] = value
        power = value * value
        part = squares[r - 1]
        for top in range(0, layers, TILE):
            for start in range(0, WIDTH, PAD):
                part = part + power[top : top + TILE, start : start + PAD]
        squares[r - 1] = part

    def sweep_twice(r, c):
        inner = pl.ds(c + PAD, WIDTH)
        middle, around = in_plane(second, r, c, *second_ends(r, c))
        across = second[r - 1, body_layers, inner] + second[r + 1, body_layers, inner]
        tally(r, c, weigh(middle, across + around))

    reach = (jnp.float32(SIDE_WEIGHT), jnp.where(has_outer, SIDE_WEIGHT, 0.0))

    def prepare(flow, c):
        inner = pl.ds(c + PAD, WIDTH)
        edge = edges[flow]
        middle, around = in_plane(second, edge, c, *second_ends(edge, c))
        around = around + second[inners[flow], body_layers, inner]
        facing_own = reach[flow] * first[edge, body_layers, inner]
        field[edge - 1, :, pl.ds(c, WIDTH)] = weigh(middle, around + facing_own)

    def finish(flow, c):
        cols = pl.ds(c, WIDTH)
        edge = edges[flow]
        tally(edge, c, field[edge - 1, :, cols] + SIDE_WEIGHT * theirs[flow, :, cols])

    def over(low, count, visit):
        def body(t, carry):
            for step in range(steps):
                visit(t, step * WIDTH)
            return carry

        lax.fori_loop(low, low + count, body, 0)

    with jax.named_scope("p07_widen"):
        over(1, 2, widen)
        over(rows - 1, 2, widen)
        for c in range(RAW[PARTNER], CHUNKS):
            partner_copies[c].start()
    with jax.named_scope("p08_waitraw"):
        wait_layers(edge_layers(first, 0))
    with jax.named_scope("p09_partial"):
        for flow in (OUTER, PARTNER):
            for step in range(steps):
                partial(flow, step * WIDTH)
    with jax.named_scope("p10_fwd0"):
        forward(0)
    with jax.named_scope("p11_widen"):
        over(3, rows - 4, widen)
        for c in range(CHUNKS, 2 * CHUNKS):
            send_detour(c)
        partner_copies[CHUNKS].start()
    with jax.named_scope("p12_waitraw"):
        wait_layers(raw_layers[2])
    middle_row = rows // 2 + 1
    with jax.named_scope("p13_sweep1"):
        over(2, middle_row - 2, sweep_once)
    with jax.named_scope("p14_fwd1"):
        partner_copies[CHUNKS + 1].start()
        for c in (CHUNKS, CHUNKS + 1):
            send_direct(c)
        forward(1)
        forward(2)
    with jax.named_scope("p15_sweep1"):
        over(middle_row, rows - middle_row, sweep_once)
        start_layers(later_layers[2])
    with jax.named_scope("p16_fwd3"):
        for c in range(CHUNKS + 2, 2 * CHUNKS):
            partner_copies[c].start()
            send_direct(c)
        forward(3)
    with jax.named_scope("p16_fwds"):
        pl.when(has_beyond)(forward_shift)
    with jax.named_scope("p17_waitshift"):
        shift_partner[0].wait_recv()
        pl.when(has_outer)(shift_forward[0].wait_recv)
    for flow in (PARTNER, OUTER):

        def arrive(flow=flow):
            whole_plane(flow).wait_recv()
            for step in range(RAW[flow] * per_piece):
                widen(halos[flow], step * WIDTH)

        with jax.named_scope(f"p18_{flow}{'po'[flow]}"):
            if flow == PARTNER:
                arrive()
            else:
                pl.when(has_outer)(arrive)
            for step in range(steps):
                complete(flow, step * WIDTH)
    with jax.named_scope("p19_edges"):
        for j in (0, 1):
            start_layers(later_layers[j])
    with jax.named_scope("p20_waitlater"):
        wait_layers(later_layers[2])
    with jax.named_scope("p22_sweep2"):
        over(2, middle_row - 2, sweep_twice)
        over(middle_row, rows - middle_row, sweep_twice)
    with jax.named_scope("p23_waitlater"):
        forward(CHUNKS)
        forward(CHUNKS + 1)
        wait_layers(edge_layers(second, 2))
    with jax.named_scope("p24_prepare"):
        for flow in (PARTNER, OUTER):
            for step in range(steps):
                prepare(flow, step * WIDTH)
        for c in range(CHUNKS + 2, 2 * CHUNKS):
            forward(c)

    for k in range(CHUNKS):
        with jax.named_scope(f"p25_finish{k}"):
            for flow in (PARTNER, OUTER):
                if flow == PARTNER:
                    partner_copies[CHUNKS + k].wait_recv()
                else:
                    pl.when(has_outer)(outward_copies[CHUNKS + k].wait_recv)
                for j in range(per_piece):
                    finish(flow, k * piece + j * WIDTH)

    sums[...] = jnp.sum(squares[...], axis=1)
    for copy in sum_copies:
        copy.start()
    shift_partner[0].wait_send()
    pl.when(has_outer)(shift_detour[0].wait_send)
    pl.when(has_beyond)(shift_forward[0].wait_send)
    for side in (0, 1):
        pl.when(lat_sends[side])(surf_copies[side].wait_send)
        sent = first.at[pl.ds(1, rows), pl.ds(TILE, 2), body_cols]
        pl.when(depth_sends[side])(vertical(side, 0, sent, sent).wait_send)

    def sent_planes(flow):
        return remote(mine, mine, plane_send.at[flow], plane_recv.at[flow, 0], lat_id(partner))

    sent_planes(PARTNER).wait_send()
    pl.when(has_outer)(sent_planes(OUTER).wait_send)
    for count in sorted({(2 * CHUNKS * k) // pairs for k in range(1, pairs)} - {0}):
        passed = relay.at[pl.ds(0, count)]
        whole = remote(passed, passed, forward_send.at[0], relay_recv.at[0], lat_id(beyond))
        pl.when(relay_share == count)(whole.wait_send)
    with jax.named_scope("p27_waitsums"):
        if depths > 1:
            whole = remote(others, others, sum_send.at[0], sum_recv.at[0], {"depth": depth})
            whole.wait()
    with jax.named_scope("p28_total"):
        total = sums[...]
        for k in range(depths - 1):
            total = total + others[k]
        norm[...] = total


def deliver(count, surface_in, field_in, total, surface_out, field_out, norm_out, packed, sem):
    copies = [
        pltpu.make_async_copy(field_in, field_out, sem.at[0]),
        pltpu.make_async_copy(surface_in, surface_out, sem.at[1]),
        pltpu.make_async_copy(packed, norm_out, sem.at[2]),
    ]
    for copy in copies[:2]:
        copy.start()
    rows, lanes = total.shape[0], pl.cdiv(total.shape[0], PAD) * PAD
    column = jnp.broadcast_to(jnp.sum(total[...], axis=1, keepdims=True), (rows, lanes))
    ids = lax.broadcasted_iota(jnp.int32, column.shape, 0)
    places = lax.broadcasted_iota(jnp.int32, column.shape, 1)
    flat = jnp.sum(jnp.where(ids == places, column, 0.0), axis=0, keepdims=True)
    packed[...] = jnp.sqrt(flat / count)[0, :rows]
    copies[2].start()
    for copy in copies:
        copy.wait()


def solution(mesh):
    lats, depths = mesh.shape["lat"], mesh.shape["depth"]

    def per_device(surface, velocity, block_map, free_flags, block_rates, previous_mesh):
        rows, layers, columns = previous_mesh.shape
        wide = columns + 2 * PAD
        anywhere = pl.BlockSpec(memory_space=pltpu.HBM)
        f32 = jnp.float32
        others = max(depths - 1, 1)
        most = max((2 * CHUNKS * (lats // 2 - 1)) // (lats // 2), 1)
        dma = pltpu.SemaphoreType.DMA
        held = [
            pltpu.with_memory_space_constraint(value, pltpu.HBM)
            for value in (surface, velocity, block_map, free_flags, previous_mesh)
        ]
        results = pl.pallas_call(
            functools.partial(kernel, lats, depths),
            out_shape=(
                pltpu.VMEM(surface.shape, f32),
                pltpu.VMEM(previous_mesh.shape, f32),
                pltpu.VMEM((rows, PAD), f32),
            ),
            in_specs=[anywhere] * 4 + [pl.BlockSpec(memory_space=pltpu.SMEM), anywhere],
            out_specs=(pl.BlockSpec(memory_space=pltpu.VMEM),) * 3,
            scratch_shapes=[
                pltpu.VMEM((rows + 2 * TILE, wide), f32),
                pltpu.VMEM(velocity.shape, f32),
                pltpu.VMEM(block_map.shape, jnp.int32),
                pltpu.VMEM(free_flags.shape, jnp.int32),
                pltpu.VMEM((rows + 2 * TILE, columns), f32),
                pltpu.VMEM((rows + 2, layers + 2 * TILE, wide), f32),
                pltpu.VMEM((rows + 2, layers + 2 * TILE, wide), f32),
                pltpu.VMEM((2, layers, columns), f32),
                pltpu.VMEM((2, layers, columns), f32),
                pltpu.VMEM((most, layers, columns // CHUNKS), f32),
                pltpu.VMEM((1, RAW[OUTER] * (columns // CHUNKS)), f32),
                pltpu.VMEM((rows, TILE, PAD), f32),
                pltpu.VMEM((rows, PAD), f32),
                pltpu.VMEM((others, rows, PAD), f32),
                dma((5,)),
                dma((2,)),
                dma((2,)),
                dma((3,)),
                dma((3,)),
                dma((2,)),
                dma((2, 1 + CHUNKS)),
                dma((most,)),
                dma((1,)),
                dma((2,)),
                dma((2, 4)),
                dma((1,)),
                dma((1,)),
            ],
            compiler_params=pltpu.CompilerParams(
                collective_id=0, has_side_effects=True, vmem_limit_bytes=56 * 1024 * 1024
            ),
            name="advect_and_relax",
        )(*held[:4], block_rates, held[4])
        resident = [pltpu.with_memory_space_constraint(value, pltpu.VMEM) for value in results]
        new_surface, field, norm = pl.pallas_call(
            functools.partial(deliver, layers * depths * columns),
            out_shape=(
                pltpu.HBM(surface.shape, f32),
                pltpu.HBM(previous_mesh.shape, f32),
                pltpu.HBM((rows,), f32),
            ),
            in_specs=[pl.BlockSpec(memory_space=pltpu.VMEM)] * 3,
            out_specs=(anywhere,) * 3,
            scratch_shapes=[pltpu.VMEM((rows,), f32), dma((3,))],
            compiler_params=pltpu.CompilerParams(vmem_limit_bytes=1024 * 1024),
            name="deliver",
        )(*resident)
        return new_surface, field, norm

    return jax.shard_map(
        per_device,
        mesh=mesh,
        in_specs=(
            P("lat", None),
            P(None, "lat", None),
            P("lat", None),
            P("lat", None),
            P(),
            P("lat", "depth", None),
        ),
        out_specs=(P("lat", None), P("lat", "depth", None), P("lat")),
        check_vma=False,
    )
```

```python
import functools

import jax
import jax.numpy as jnp
from jax import lax
from jax.experimental import pallas as pl
from jax.experimental.pallas import tpu as pltpu
from jax.sharding import PartitionSpec as P

ITERS = 2
TIME_STEP = 0.5
RELAX_WEIGHT = 0.8
SIDE_WEIGHT = RELAX_WEIGHT / 6.0
MESH = pl.DeviceIdType.MESH
PAD = 128
TILE = 8
WIDTH = 1024
CHUNKS = 4
RAW = (2, 2)
PARTNER, OUTER = 0, 1


def lanes_beside(window, width):
    span = window.shape[1]
    left = pltpu.roll(window, 1, 1)[:, PAD : PAD + width]
    right = pltpu.roll(window, span - 1, 1)[:, PAD : PAD + width]
    return window[:, PAD : PAD + width], left, right


def kernel(
    lats,
    depths,
    surface,
    velocity,
    block_map,
    free_flags,
    block_rates,
    previous,
    new_surface,
    field,
    norm,
    surf,
    vel,
    blocks,
    flags,
    rates,
    shift,
    first,
    second,
    mine,
    theirs,
    relay,
    relay_shift,
    squares,
    sums,
    others,
    local_sem,
    near_send,
    near_recv,
    shift_send,
    shift_recv,
    plane_send,
    plane_recv,
    relay_recv,
    forward_send,
    depth_send,
    depth_recv,
    sum_send,
    sum_recv,
):
    rows, layers, columns = previous.shape
    lat = lax.axis_index("lat")
    depth = lax.axis_index("depth")
    total_layers = layers * depths
    blocks_count = block_rates.shape[0]
    steps = columns // WIDTH
    piece = columns // CHUNKS
    per_piece = piece // WIDTH
    has_low, has_high = lat > 0, lat < lats - 1
    has_above, has_below = depth > 0, depth < depths - 1
    body_rows = pl.ds(TILE, rows)
    body_layers = pl.ds(TILE, layers)
    body_cols = pl.ds(PAD, columns)

    odd = lax.rem(lat, 2)
    pair, pairs = lat // 2, lats // 2
    partner = lat + 1 - 2 * odd
    outward = lat - 1 + 2 * odd
    beyond = lat + 2 - 4 * odd
    behind = lat - 2 + 4 * odd
    has_outer = jnp.logical_and(outward >= 0, outward < lats)
    has_beyond = jnp.logical_and(beyond >= 0, beyond < lats)
    down_share = (2 * CHUNKS * pair) // pairs
    up_share = (2 * CHUNKS * (pairs - 1 - pair)) // pairs - lax.rem(depth, 2)
    up_share = jnp.maximum(up_share, 0)
    own_share = jnp.where(odd == 0, down_share, up_share)
    relay_share = jnp.where(odd == 0, up_share, down_share)
    low_side, high_side = odd, 1 - odd
    edges = (1 + (rows - 1) * high_side, 1 + (rows - 1) * low_side)
    inners = (2 + (rows - 3) * high_side, 2 + (rows - 3) * low_side)
    halos = ((rows + 1) * high_side, (rows + 1) * low_side)

    local_surface = pltpu.make_async_copy(
        surface, surf.at[body_rows, body_cols], local_sem.at[0]
    )
    local_inputs = [
        pltpu.make_async_copy(velocity, vel, local_sem.at[1]),
        pltpu.make_async_copy(block_map, blocks, local_sem.at[2]),
        pltpu.make_async_copy(free_flags, flags, local_sem.at[3]),
        pltpu.make_async_copy(block_rates, rates, local_sem.at[5]),
    ]
    local_mesh = pltpu.make_async_copy(
        previous, first.at[pl.ds(1, rows), body_layers, body_cols], local_sem.at[4]
    )

    barrier = pltpu.get_barrier_semaphore()

    def greet(target):
        pl.semaphore_signal(barrier, inc=1, device_id=target, device_id_type=MESH)

    def lat_id(index):
        return {"lat": jnp.clip(index, 0, lats - 1)}

    greet(lat_id(partner))
    pl.when(has_outer)(lambda: greet(lat_id(outward)))
    pl.when(has_beyond)(lambda: greet(lat_id(beyond)))
    pl.when(has_outer)(lambda: greet(lat_id(behind)))
    for k in range(1, depths):
        greet({"depth": lax.rem(depth + k, depths)})
    for copy in [local_surface]:
        copy.start()
    peers = depths + 2 * has_outer.astype(jnp.int32) + has_beyond.astype(jnp.int32)
    with jax.named_scope("p01_barrier"):
        pl.semaphore_wait(barrier, peers)

    def remote(src, dst, send, recv, target):
        return pltpu.make_async_remote_copy(
            src_ref=src,
            dst_ref=dst,
            send_sem=send,
            recv_sem=recv,
            device_id=target,
            device_id_type=MESH,
        )

    def nearby(side, src, dst):
        target = lat_id(lat + 1 if side == 0 else lat - 1)
        return remote(src, dst, near_send.at[side], near_recv.at[side], target)

    def vertical(side, slot, src, dst):
        index = depth + 1 if side == 0 else depth - 1
        target = {"depth": jnp.clip(index, 0, depths - 1)}
        return remote(src, dst, depth_send.at[side], depth_recv.at[side, slot], target)

    def piece_cols(k, pad=0):
        return pl.ds(pad + k * piece, piece)

    lat_sends = (has_high, has_low)
    lat_recvs = (has_low, has_high)
    depth_sends = (has_below, has_above)
    depth_recvs = (has_above, has_below)
    own_layer = (TILE + layers - 1, TILE)
    far_layer = (TILE - 1, TILE + layers)
    own_row = (TILE + rows - 1, TILE)
    far_row = (TILE - 1, TILE + rows)

    surf_copies = [
        nearby(
            side,
            surf.at[pl.ds(own_row[side], 1), body_cols],
            surf.at[pl.ds(far_row[side], 1), body_cols],
        )
        for side in (0, 1)
    ]

    def shift_row(row, flow):
        return shift.at[pl.ds(row, 1), pl.ds(0, RAW[flow] * piece)]

    shift_partner = [
        remote(
            shift_row(own_row[side], PARTNER),
            shift_row(far_row[side], PARTNER),
            shift_send.at[0],
            shift_recv.at[0],
            lat_id(partner),
        )
        for side in (0, 1)
    ]
    shift_detour = [
        remote(
            shift_row(own_row[side], OUTER),
            relay_shift,
            shift_send.at[1],
            shift_recv.at[1],
            lat_id(partner),
        )
        for side in (0, 1)
    ]
    shift_forward = [
        remote(
            relay_shift,
            shift_row(far_row[side], OUTER),
            shift_send.at[2],
            shift_recv.at[2],
            lat_id(beyond),
        )
        for side in (0, 1)
    ]

    def send_shift():
        for side in (0, 1):
            toward = (odd == 0) if side == 0 else (odd == 1)
            away = jnp.logical_and(has_outer, (odd == 1) if side == 0 else (odd == 0))
            pl.when(away)(shift_detour[side].start)
            pl.when(toward)(shift_partner[side].start)

    def forward_shift():
        shift_detour[0].wait_recv()
        for side in (0, 1):
            pl.when((odd == 0) if side == 0 else (odd == 1))(shift_forward[side].start)

    def source(flow, c):
        if c < RAW[flow]:
            return previous.at[edges[flow] - 1, :, piece_cols(c)]
        if c < CHUNKS:
            return first.at[edges[flow], body_layers, piece_cols(c, PAD)]
        return mine.at[flow, :, piece_cols(c - CHUNKS)]

    def landing(flow, halo, c):
        if c < CHUNKS:
            return first.at[halo, body_layers, piece_cols(c, PAD)]
        return theirs.at[flow, :, piece_cols(c - CHUNKS)]

    partner_halo = (rows + 1) * low_side
    outward_halo = (rows + 1) * high_side
    beyond_halo = (rows + 1) * low_side
    pieces = range(2 * CHUNKS)
    order = list(pieces)
    most = (2 * CHUNKS * (pairs - 1)) // pairs
    detours = order[:most]

    def landed(flow, c):
        return plane_recv.at[flow, max(c - CHUNKS + 1, 0)]

    partner_copies = [
        remote(
            source(PARTNER, c),
            landing(PARTNER, partner_halo, c),
            plane_send.at[PARTNER],
            landed(PARTNER, c),
            lat_id(partner),
        )
        for c in pieces
    ]
    outward_copies = [
        remote(
            source(OUTER, c),
            landing(OUTER, outward_halo, c),
            plane_send.at[OUTER],
            landed(OUTER, c),
            lat_id(outward),
        )
        for c in pieces
    ]
    detour_copies = {
        c: remote(
            source(OUTER, c),
            relay.at[slot],
            plane_send.at[OUTER],
            relay_recv.at[slot],
            lat_id(partner),
        )
        for slot, c in enumerate(detours)
    }
    forward_copies = {
        c: remote(
            relay.at[slot],
            landing(OUTER, beyond_halo, c),
            forward_send.at[0],
            landed(OUTER, c),
            lat_id(beyond),
        )
        for slot, c in enumerate(detours)
    }

    def whole_plane(flow):
        whole = first.at[halos[flow], body_layers, body_cols]
        return remote(whole, whole, plane_send.at[flow], plane_recv.at[flow, 0], lat_id(partner))

    def send_detour(c):
        if c in detour_copies:
            pl.when(own_share > detours.index(c))(detour_copies[c].start)

    def send_direct(c):
        direct = has_outer
        if c in detour_copies:
            direct = jnp.logical_and(has_outer, own_share <= detours.index(c))
        pl.when(direct)(outward_copies[c].start)

    def forward(c):
        if c not in forward_copies:
            return

        @pl.when(relay_share > detours.index(c))
        def _():
            detour_copies[c].wait_recv()
            forward_copies[c].start()

    spans = (pl.ds(1, 1), pl.ds(rows, 1), pl.ds(2, rows - 2))
    raw_spans = (pl.ds(0, 1), pl.ds(rows - 1, 1), pl.ds(1, rows - 2))
    raw_layers = [
        [
            vertical(
                side,
                min(j, 2) // 2,
                previous.at[raw, pl.ds((layers - 1, 0)[side], 1), :],
                first.at[span, pl.ds(far_layer[side], 1), body_cols],
            )
            for side in (0, 1)
        ]
        for j, (raw, span) in enumerate(zip(raw_spans, spans))
    ]
    later_layers = [
        [
            vertical(
                side,
                2 + min(j, 2) // 2,
                second.at[span, pl.ds(own_layer[side], 1), body_cols],
                second.at[span, pl.ds(far_layer[side], 1), body_cols],
            )
            for side in (0, 1)
        ]
        for j, span in enumerate(spans)
    ]

    def edge_layers(buffer, slot):
        pair_span = pl.ds(1, 2)
        return [
            vertical(side, slot, *[buffer.at[pair_span, pl.ds(far_layer[side], 1), body_cols]] * 2)
            for side in (0, 1)
        ]

    sum_copies = [
        remote(
            sums,
            others.at[k - 1],
            sum_send.at[0],
            sum_recv.at[0],
            {"depth": lax.rem(depth + k, depths)},
        )
        for k in range(1, depths)
    ]

    def start_layers(group):
        for side in (0, 1):
            pl.when(depth_sends[side])(group[side].start)

    def wait_layers(group):
        for side in (0, 1):
            pl.when(depth_recvs[side])(group[side].wait_recv)

    with jax.named_scope("p02_sends"):
        local_surface.wait()
        for side in (0, 1):
            pl.when(lat_sends[side])(surf_copies[side].start)
        for group in raw_layers[:2]:
            start_layers(group)
        for c in range(RAW[OUTER]):
            send_detour(c)
        for c in range(RAW[PARTNER]):
            partner_copies[c].start()
        for c in range(RAW[OUTER]):
            send_direct(c)
        start_layers(raw_layers[2])

    for copy in [*local_inputs, local_mesh]:
        copy.start()
    zero_tile = jnp.zeros((layers, PAD), jnp.float32)

    def clear_pads(r, carry):
        for buffer in (first, second):
            for start in (0, PAD + columns):
                buffer[r, body_layers, pl.ds(start, PAD)] = zero_tile
        return carry

    lax.fori_loop(1, rows + 1, clear_pads, 0)
    for start in (0, PAD + columns):
        surf[body_rows, pl.ds(start, PAD)] = jnp.zeros((rows, PAD), jnp.float32)
    squares[...] = jnp.zeros_like(squares)

    for side in (0, 1):

        @pl.when(jnp.logical_not(lat_recvs[side]))
        def _(side=side):
            surf[pl.ds(far_row[side], 1), body_cols] = jnp.zeros((1, columns), jnp.float32)
            shift[pl.ds(far_row[side], 1), :] = jnp.zeros((1, columns), jnp.float32)
            first[(0, rows + 1)[side], body_layers, body_cols] = jnp.zeros(
                (layers, columns), jnp.float32
            )
            theirs[OUTER] = jnp.zeros((layers, columns), jnp.float32)

    with jax.named_scope("p04_waitsurf"):
        for copy in local_inputs:
            copy.wait()
        for side in (0, 1):
            pl.when(lat_recvs[side])(surf_copies[side].wait_recv)

    def advect(step, carry):
        c = pl.multiple_of(step * WIDTH, WIDTH)
        cols = pl.ds(c, WIDTH)
        inner = pl.ds(pl.multiple_of(c + PAD, PAD), WIDTH)
        middle, left, right = lanes_beside(surf[body_rows, pl.ds(c, WIDTH + 2 * PAD)], WIDTH)
        before = pltpu.roll(surf[pl.ds(0, rows + TILE), inner], 1, 0)[TILE:]
        after = pltpu.roll(surf[pl.ds(TILE, rows + TILE), inner], rows + TILE - 1, 0)[:rows]
        grad_rows = (after - before) * 0.5
        grad_cols = (right - left) * 0.5
        laplace = after + before + right + left - 4.0 * middle
        names = blocks[:, cols]
        rate = jnp.full(names.shape, rates[0], jnp.float32)
        for label in range(1, blocks_count):
            rate = jnp.where(names == label, rates[label], rate)
        tendency = -vel[0, :, cols] * grad_rows - vel[1, :, cols] * grad_cols + rate * laplace
        fresh = middle + TIME_STEP * flags[:, cols].astype(jnp.float32) * tendency
        new_surface[:, cols] = fresh
        shift[body_rows, cols] = fresh - middle
        return carry

    with jax.named_scope("p05_advect"):
        lax.fori_loop(0, steps, advect, 0)
    with jax.named_scope("p06_sends"):
        send_shift()
        local_mesh.wait()

    def profile_of(index):
        return (total_layers - index).astype(jnp.float32) / total_layers

    base = depth * layers
    profile = profile_of(base + lax.broadcasted_iota(jnp.int32, (layers, PAD), 0))
    above_profile = profile_of(base - 1)
    below_profile = profile_of(base + layers)
    sublane = lax.broadcasted_iota(jnp.int32, (layers, WIDTH), 0)
    at_first = sublane == 0
    at_last = sublane == layers - 1
    above = pl.ds(TILE - 1, 1)
    below = pl.ds(TILE + layers, 1)

    def widen(r, c):
        inner = pl.ds(c + PAD, WIDTH)
        row_shift = jnp.broadcast_to(shift[pl.ds(TILE - 1 + r, 1), pl.ds(c, WIDTH)], (layers, WIDTH))
        wide_profile = jnp.concatenate([profile] * (WIDTH // PAD), axis=1)
        first[r, body_layers, inner] = first[r, body_layers, inner] + row_shift * wide_profile

    def in_plane(source, r, c, top, bottom):
        middle, left, right = lanes_beside(
            source[r, body_layers, pl.ds(c, WIDTH + 2 * PAD)], WIDTH
        )
        upper = jnp.where(at_first, top, pltpu.roll(middle, 1, 0))
        lower = jnp.where(at_last, bottom, pltpu.roll(middle, layers - 1, 0))
        return middle, (left + right) + (upper + lower)

    def first_ends(r, c):
        inner = pl.ds(c + PAD, WIDTH)
        row_shift = shift[pl.ds(TILE - 1 + r, 1), pl.ds(c, WIDTH)]
        top = jnp.where(has_above, first[r, above, inner] + row_shift * above_profile, row_shift)
        bottom = jnp.where(has_below, first[r, below, inner] + row_shift * below_profile, 0.0)
        return top, bottom

    def second_ends(r, c):
        inner = pl.ds(c + PAD, WIDTH)
        row_shift = shift[pl.ds(TILE - 1 + r, 1), pl.ds(c, WIDTH)]
        top = jnp.where(has_above, second[r, above, inner], row_shift)
        bottom = jnp.where(has_below, second[r, below, inner], 0.0)
        return top, bottom

    def weigh(middle, neighbours):
        return (1.0 - RELAX_WEIGHT) * middle + SIDE_WEIGHT * neighbours

    def partial(flow, c):
        inner = pl.ds(c + PAD, WIDTH)
        middle, around = in_plane(first, edges[flow], c, *first_ends(edges[flow], c))
        mine[flow, :, pl.ds(c, WIDTH)] = weigh(
            middle, around + first[inners[flow], body_layers, inner]
        )

    def complete(flow, c):
        inner = pl.ds(c + PAD, WIDTH)
        second[edges[flow], body_layers, inner] = (
            mine[flow, :, pl.ds(c, WIDTH)] + SIDE_WEIGHT * first[halos[flow], body_layers, inner]
        )

    def sweep_once(r, c):
        inner = pl.ds(c + PAD, WIDTH)
        middle, around = in_plane(first, r, c, *first_ends(r, c))
        across = first[r - 1, body_layers, inner] + first[r + 1, body_layers, inner]
        second[r, body_layers, inner] = weigh(middle, across + around)

    def tally(r, c, value):
        field[r - 1, :, pl.ds(c, WIDTH)] = value
        power = value * value
        part = squares[r - 1]
        for top in range(0, layers, TILE):
            for start in range(0, WIDTH, PAD):
                part = part + power[top : top + TILE, start : start + PAD]
        squares[r - 1] = part

    def sweep_twice(r, c):
        inner = pl.ds(c + PAD, WIDTH)
        middle, around = in_plane(second, r, c, *second_ends(r, c))
        across = second[r - 1, body_layers, inner] + second[r + 1, body_layers, inner]
        tally(r, c, weigh(middle, across + around))

    reach = (jnp.float32(SIDE_WEIGHT), jnp.where(has_outer, SIDE_WEIGHT, 0.0))

    def prepare(flow, c):
        inner = pl.ds(c + PAD, WIDTH)
        edge = edges[flow]
        middle, around = in_plane(second, edge, c, *second_ends(edge, c))
        around = around + second[inners[flow], body_layers, inner]
        facing_own = reach[flow] * first[edge, body_layers, inner]
        field[edge - 1, :, pl.ds(c, WIDTH)] = weigh(middle, around + facing_own)

    def finish(flow, c):
        cols = pl.ds(c, WIDTH)
        edge = edges[flow]
        tally(edge, c, field[edge - 1, :, cols] + SIDE_WEIGHT * theirs[flow, :, cols])

    def over(low, count, visit):
        def body(t, carry):
            for step in range(steps):
                visit(t, step * WIDTH)
            return carry

        lax.fori_loop(low, low + count, body, 0)

    with jax.named_scope("p07_widen"):
        over(1, 2, widen)
        over(rows - 1, 2, widen)
        for c in range(RAW[OUTER], CHUNKS):
            send_detour(c)
        for c in range(RAW[PARTNER], CHUNKS):
            partner_copies[c].start()
        for c in range(RAW[OUTER], CHUNKS):
            send_direct(c)
    with jax.named_scope("p08_waitraw"):
        wait_layers(edge_layers(first, 0))
    with jax.named_scope("p09_partial"):
        for flow in (OUTER, PARTNER):
            for step in range(steps):
                partial(flow, step * WIDTH)
    with jax.named_scope("p10_fwd0"):
        forward(0)
    with jax.named_scope("p11_widen"):
        over(3, rows - 4, widen)
        for c in range(CHUNKS, 2 * CHUNKS):
            send_detour(c)
        partner_copies[CHUNKS].start()
    with jax.named_scope("p12_waitraw"):
        wait_layers(raw_layers[2])
    middle_row = rows // 2 + 1
    with jax.named_scope("p13_sweep1"):
        over(2, middle_row - 2, sweep_once)
    with jax.named_scope("p14_fwd1"):
        partner_copies[CHUNKS + 1].start()
        for c in (CHUNKS, CHUNKS + 1):
            send_direct(c)
        forward(1)
    with jax.named_scope("p15_sweep1"):
        over(middle_row, rows - middle_row, sweep_once)
        start_layers(later_layers[2])
    with jax.named_scope("p16_fwd3"):
        for c in range(CHUNKS + 2, 2 * CHUNKS):
            partner_copies[c].start()
            send_direct(c)
        forward(2)
        forward(3)
    with jax.named_scope("p16_fwds"):
        pl.when(has_beyond)(forward_shift)
    with jax.named_scope("p17_waitshift"):
        shift_partner[0].wait_recv()
        pl.when(has_outer)(shift_forward[0].wait_recv)
    for flow in (PARTNER, OUTER):

        def arrive(flow=flow):
            whole_plane(flow).wait_recv()
            for step in range(RAW[flow] * per_piece):
                widen(halos[flow], step * WIDTH)

        with jax.named_scope(f"p18_{flow}{'po'[flow]}"):
            if flow == PARTNER:
                arrive()
            else:
                pl.when(has_outer)(arrive)
            for step in range(steps):
                complete(flow, step * WIDTH)
    with jax.named_scope("p19_edges"):
        for j in (0, 1):
            start_layers(later_layers[j])
    with jax.named_scope("p20_waitlater"):
        wait_layers(later_layers[2])
    with jax.named_scope("p22_sweep2"):
        over(2, middle_row - 2, sweep_twice)
        over(middle_row, rows - middle_row, sweep_twice)
    with jax.named_scope("p23_waitlater"):
        forward(CHUNKS)
        forward(CHUNKS + 1)
        wait_layers(edge_layers(second, 2))
    with jax.named_scope("p24_prepare"):
        for flow in (PARTNER, OUTER):
            for step in range(steps):
                prepare(flow, step * WIDTH)
        for c in range(CHUNKS + 2, 2 * CHUNKS):
            forward(c)

    for k in range(CHUNKS):
        with jax.named_scope(f"p25_finish{k}"):
            for flow in (PARTNER, OUTER):
                if flow == PARTNER:
                    partner_copies[CHUNKS + k].wait_recv()
                else:
                    pl.when(has_outer)(outward_copies[CHUNKS + k].wait_recv)
                for j in range(per_piece):
                    finish(flow, k * piece + j * WIDTH)

    sums[...] = jnp.sum(squares[...], axis=1)
    for copy in sum_copies:
        copy.start()
    shift_partner[0].wait_send()
    pl.when(has_outer)(shift_detour[0].wait_send)
    pl.when(has_beyond)(shift_forward[0].wait_send)
    for side in (0, 1):
        pl.when(lat_sends[side])(surf_copies[side].wait_send)
        sent = first.at[pl.ds(1, rows), pl.ds(TILE, 2), body_cols]
        pl.when(depth_sends[side])(vertical(side, 0, sent, sent).wait_send)

    def sent_planes(flow):
        return remote(mine, mine, plane_send.at[flow], plane_recv.at[flow, 0], lat_id(partner))

    sent_planes(PARTNER).wait_send()
    pl.when(has_outer)(sent_planes(OUTER).wait_send)
    for count in range(1, most + 1):
        passed = relay.at[pl.ds(0, count)]
        whole = remote(passed, passed, forward_send.at[0], relay_recv.at[0], lat_id(beyond))
        pl.when(relay_share == count)(whole.wait_send)
    with jax.named_scope("p27_waitsums"):
        if depths > 1:
            whole = remote(others, others, sum_send.at[0], sum_recv.at[0], {"depth": depth})
            whole.wait()
    with jax.named_scope("p28_total"):
        total = sums[...]
        for k in range(depths - 1):
            total = total + others[k]
        norm[...] = total


def deliver(count, surface_in, field_in, total, surface_out, field_out, norm_out, packed, sem):
    copies = [
        pltpu.make_async_copy(field_in, field_out, sem.at[0]),
        pltpu.make_async_copy(surface_in, surface_out, sem.at[1]),
        pltpu.make_async_copy(packed, norm_out, sem.at[2]),
    ]
    for copy in copies[:2]:
        copy.start()
    rows, lanes = total.shape[0], pl.cdiv(total.shape[0], PAD) * PAD
    column = jnp.broadcast_to(jnp.sum(total[...], axis=1, keepdims=True), (rows, lanes))
    ids = lax.broadcasted_iota(jnp.int32, column.shape, 0)
    places = lax.broadcasted_iota(jnp.int32, column.shape, 1)
    flat = jnp.sum(jnp.where(ids == places, column, 0.0), axis=0, keepdims=True)
    packed[...] = jnp.sqrt(flat / count)[0, :rows]
    copies[2].start()
    for copy in copies:
        copy.wait()


def solution(mesh):
    lats, depths = mesh.shape["lat"], mesh.shape["depth"]

    def per_device(surface, velocity, block_map, free_flags, block_rates, previous_mesh):
        rows, layers, columns = previous_mesh.shape
        wide = columns + 2 * PAD
        anywhere = pl.BlockSpec(memory_space=pltpu.HBM)
        f32 = jnp.float32
        others = max(depths - 1, 1)
        most = max((2 * CHUNKS * (lats // 2 - 1)) // (lats // 2), 1)
        dma = pltpu.SemaphoreType.DMA
        held = [
            pltpu.with_memory_space_constraint(value, pltpu.HBM)
            for value in (surface, velocity, block_map, free_flags, block_rates, previous_mesh)
        ]
        results = pl.pallas_call(
            functools.partial(kernel, lats, depths),
            out_shape=(
                pltpu.VMEM(surface.shape, f32),
                pltpu.VMEM(previous_mesh.shape, f32),
                pltpu.VMEM((rows, PAD), f32),
            ),
            in_specs=[anywhere] * 6,
            out_specs=(pl.BlockSpec(memory_space=pltpu.VMEM),) * 3,
            scratch_shapes=[
                pltpu.VMEM((rows + 2 * TILE, wide), f32),
                pltpu.VMEM(velocity.shape, f32),
                pltpu.VMEM(block_map.shape, jnp.int32),
                pltpu.VMEM(free_flags.shape, jnp.int32),
                pltpu.SMEM(block_rates.shape, f32),
                pltpu.VMEM((rows + 2 * TILE, columns), f32),
                pltpu.VMEM((rows + 2, layers + 2 * TILE, wide), f32),
                pltpu.VMEM((rows + 2, layers + 2 * TILE, wide), f32),
                pltpu.VMEM((2, layers, columns), f32),
                pltpu.VMEM((2, layers, columns), f32),
                pltpu.VMEM((most, layers, columns // CHUNKS), f32),
                pltpu.VMEM((1, RAW[OUTER] * (columns // CHUNKS)), f32),
                pltpu.VMEM((rows, TILE, PAD), f32),
                pltpu.VMEM((rows, PAD), f32),
                pltpu.VMEM((others, rows, PAD), f32),
                dma((6,)),
                dma((2,)),
                dma((2,)),
                dma((3,)),
                dma((3,)),
                dma((2,)),
                dma((2, 1 + CHUNKS)),
                dma((most,)),
                dma((1,)),
                dma((2,)),
                dma((2, 4)),
                dma((1,)),
                dma((1,)),
            ],
            compiler_params=pltpu.CompilerParams(
                collective_id=0, has_side_effects=True, vmem_limit_bytes=56 * 1024 * 1024
            ),
            name="advect_and_relax",
        )(*held)
        resident = [pltpu.with_memory_space_constraint(value, pltpu.VMEM) for value in results]
        new_surface, field, norm = pl.pallas_call(
            functools.partial(deliver, layers * depths * columns),
            out_shape=(
                pltpu.HBM(surface.shape, f32),
                pltpu.HBM(previous_mesh.shape, f32),
                pltpu.HBM((rows,), f32),
            ),
            in_specs=[pl.BlockSpec(memory_space=pltpu.VMEM)] * 3,
            out_specs=(anywhere,) * 3,
            scratch_shapes=[pltpu.VMEM((rows,), f32), dma((3,))],
            compiler_params=pltpu.CompilerParams(vmem_limit_bytes=1024 * 1024),
            name="deliver",
        )(*resident)
        return new_surface, field, norm

    return jax.shard_map(
        per_device,
        mesh=mesh,
        in_specs=(
            P("lat", None),
            P(None, "lat", None),
            P("lat", None),
            P("lat", None),
            P(),
            P("lat", "depth", None),
        ),
        out_specs=(P("lat", None), P("lat", "depth", None), P("lat")),
        check_vma=False,
    )
```

```python
import functools

import jax
import jax.numpy as jnp
from jax import lax
from jax.experimental import pallas as pl
from jax.experimental.pallas import tpu as pltpu
from jax.sharding import PartitionSpec as P

ITERS = 2
TIME_STEP = 0.5
RELAX_WEIGHT = 0.8
SIDE_WEIGHT = RELAX_WEIGHT / 6.0
MESH = pl.DeviceIdType.MESH
PAD = 128
TILE = 8
WIDTH = 1024
CHUNKS = 4
RAW = (2, 2)
PARTNER, OUTER = 0, 1


def lanes_beside(window, width):
    span = window.shape[1]
    left = pltpu.roll(window, 1, 1)[:, PAD : PAD + width]
    right = pltpu.roll(window, span - 1, 1)[:, PAD : PAD + width]
    return window[:, PAD : PAD + width], left, right


def kernel(
    lats,
    depths,
    surface,
    velocity,
    block_map,
    free_flags,
    block_rates,
    previous,
    new_surface,
    field,
    norm,
    surf,
    vel,
    blocks,
    flags,
    rates,
    shift,
    first,
    second,
    mine,
    theirs,
    relay,
    relay_shift,
    squares,
    sums,
    others,
    last,
    last_others,
    local_sem,
    near_send,
    near_recv,
    shift_send,
    shift_recv,
    plane_send,
    plane_recv,
    relay_recv,
    forward_send,
    depth_send,
    depth_recv,
    sum_send,
    sum_recv,
):
    rows, layers, columns = previous.shape
    lat = lax.axis_index("lat")
    depth = lax.axis_index("depth")
    total_layers = layers * depths
    blocks_count = block_rates.shape[0]
    steps = columns // WIDTH
    piece = columns // CHUNKS
    per_piece = piece // WIDTH
    has_low, has_high = lat > 0, lat < lats - 1
    has_above, has_below = depth > 0, depth < depths - 1
    body_rows = pl.ds(TILE, rows)
    body_layers = pl.ds(TILE, layers)
    body_cols = pl.ds(PAD, columns)

    odd = lax.rem(lat, 2)
    pair, pairs = lat // 2, lats // 2
    partner = lat + 1 - 2 * odd
    outward = lat - 1 + 2 * odd
    beyond = lat + 2 - 4 * odd
    behind = lat - 2 + 4 * odd
    has_outer = jnp.logical_and(outward >= 0, outward < lats)
    has_beyond = jnp.logical_and(beyond >= 0, beyond < lats)
    down_share = (2 * CHUNKS * pair) // pairs
    up_share = (2 * CHUNKS * (pairs - 1 - pair)) // pairs - lax.rem(depth, 2)
    up_share = jnp.maximum(up_share, 0)
    own_share = jnp.where(odd == 0, down_share, up_share)
    relay_share = jnp.where(odd == 0, up_share, down_share)
    low_side, high_side = odd, 1 - odd
    edges = (1 + (rows - 1) * high_side, 1 + (rows - 1) * low_side)
    inners = (2 + (rows - 3) * high_side, 2 + (rows - 3) * low_side)
    halos = ((rows + 1) * high_side, (rows + 1) * low_side)

    local_surface = pltpu.make_async_copy(
        surface, surf.at[body_rows, body_cols], local_sem.at[0]
    )
    local_inputs = [
        pltpu.make_async_copy(velocity, vel, local_sem.at[1]),
        pltpu.make_async_copy(block_map, blocks, local_sem.at[2]),
        pltpu.make_async_copy(free_flags, flags, local_sem.at[3]),
        pltpu.make_async_copy(block_rates, rates, local_sem.at[5]),
    ]
    local_mesh = pltpu.make_async_copy(
        previous, first.at[pl.ds(1, rows), body_layers, body_cols], local_sem.at[4]
    )

    barrier = pltpu.get_barrier_semaphore()

    def greet(target):
        pl.semaphore_signal(barrier, inc=1, device_id=target, device_id_type=MESH)

    def lat_id(index):
        return {"lat": jnp.clip(index, 0, lats - 1)}

    greet(lat_id(partner))
    pl.when(has_outer)(lambda: greet(lat_id(outward)))
    pl.when(has_beyond)(lambda: greet(lat_id(beyond)))
    pl.when(has_outer)(lambda: greet(lat_id(behind)))
    for k in range(1, depths):
        greet({"depth": lax.rem(depth + k, depths)})
    for copy in [local_surface]:
        copy.start()
    peers = depths + 2 * has_outer.astype(jnp.int32) + has_beyond.astype(jnp.int32)
    with jax.named_scope("p01_barrier"):
        pl.semaphore_wait(barrier, peers)

    def remote(src, dst, send, recv, target):
        return pltpu.make_async_remote_copy(
            src_ref=src,
            dst_ref=dst,
            send_sem=send,
            recv_sem=recv,
            device_id=target,
            device_id_type=MESH,
        )

    def nearby(side, src, dst):
        target = lat_id(lat + 1 if side == 0 else lat - 1)
        return remote(src, dst, near_send.at[side], near_recv.at[side], target)

    def vertical(side, slot, src, dst):
        index = depth + 1 if side == 0 else depth - 1
        target = {"depth": jnp.clip(index, 0, depths - 1)}
        return remote(src, dst, depth_send.at[side], depth_recv.at[side, slot], target)

    def piece_cols(k, pad=0):
        return pl.ds(pad + k * piece, piece)

    lat_sends = (has_high, has_low)
    lat_recvs = (has_low, has_high)
    depth_sends = (has_below, has_above)
    depth_recvs = (has_above, has_below)
    own_layer = (TILE + layers - 1, TILE)
    far_layer = (TILE - 1, TILE + layers)
    own_row = (TILE + rows - 1, TILE)
    far_row = (TILE - 1, TILE + rows)

    surf_copies = [
        nearby(
            side,
            surf.at[pl.ds(own_row[side], 1), body_cols],
            surf.at[pl.ds(far_row[side], 1), body_cols],
        )
        for side in (0, 1)
    ]

    def shift_row(row, flow):
        return shift.at[pl.ds(row, 1), pl.ds(0, RAW[flow] * piece)]

    shift_partner = [
        remote(
            shift_row(own_row[side], PARTNER),
            shift_row(far_row[side], PARTNER),
            shift_send.at[0],
            shift_recv.at[0],
            lat_id(partner),
        )
        for side in (0, 1)
    ]
    shift_detour = [
        remote(
            shift_row(own_row[side], OUTER),
            relay_shift,
            shift_send.at[1],
            shift_recv.at[1],
            lat_id(partner),
        )
        for side in (0, 1)
    ]
    shift_forward = [
        remote(
            relay_shift,
            shift_row(far_row[side], OUTER),
            shift_send.at[2],
            shift_recv.at[2],
            lat_id(beyond),
        )
        for side in (0, 1)
    ]

    def send_shift():
        for side in (0, 1):
            toward = (odd == 0) if side == 0 else (odd == 1)
            away = jnp.logical_and(has_outer, (odd == 1) if side == 0 else (odd == 0))
            pl.when(away)(shift_detour[side].start)
            pl.when(toward)(shift_partner[side].start)

    def forward_shift():
        shift_detour[0].wait_recv()
        for side in (0, 1):
            pl.when((odd == 0) if side == 0 else (odd == 1))(shift_forward[side].start)

    def source(flow, c):
        if c < RAW[flow]:
            return previous.at[edges[flow] - 1, :, piece_cols(c)]
        if c < CHUNKS:
            return first.at[edges[flow], body_layers, piece_cols(c, PAD)]
        return mine.at[flow, :, piece_cols(c - CHUNKS)]

    def landing(flow, halo, c):
        if c < CHUNKS:
            return first.at[halo, body_layers, piece_cols(c, PAD)]
        return theirs.at[flow, :, piece_cols(c - CHUNKS)]

    partner_halo = (rows + 1) * low_side
    outward_halo = (rows + 1) * high_side
    beyond_halo = (rows + 1) * low_side
    pieces = range(2 * CHUNKS)
    order = list(pieces)
    most = (2 * CHUNKS * (pairs - 1)) // pairs
    detours = order[:most]

    def landed(flow, c):
        return plane_recv.at[flow if c < CHUNKS else 2 + c - CHUNKS]

    partner_copies = [
        remote(
            source(PARTNER, c),
            landing(PARTNER, partner_halo, c),
            plane_send.at[PARTNER],
            landed(PARTNER, c),
            lat_id(partner),
        )
        for c in pieces
    ]
    outward_copies = [
        remote(
            source(OUTER, c),
            landing(OUTER, outward_halo, c),
            plane_send.at[OUTER],
            landed(OUTER, c),
            lat_id(outward),
        )
        for c in pieces
    ]
    detour_copies = {
        c: remote(
            source(OUTER, c),
            relay.at[slot],
            plane_send.at[OUTER],
            relay_recv.at[slot],
            lat_id(partner),
        )
        for slot, c in enumerate(detours)
    }
    forward_copies = {
        c: remote(
            relay.at[slot],
            landing(OUTER, beyond_halo, c),
            forward_send.at[0],
            landed(OUTER, c),
            lat_id(beyond),
        )
        for slot, c in enumerate(detours)
    }

    def whole_plane(flow):
        whole = first.at[halos[flow], body_layers, body_cols]
        return remote(whole, whole, plane_send.at[flow], plane_recv.at[flow], lat_id(partner))

    def send_detour(c):
        if c in detour_copies:
            pl.when(own_share > detours.index(c))(detour_copies[c].start)

    def send_direct(c):
        direct = has_outer
        if c in detour_copies:
            direct = jnp.logical_and(has_outer, own_share <= detours.index(c))
        pl.when(direct)(outward_copies[c].start)

    def forward(c):
        if c not in forward_copies:
            return

        @pl.when(relay_share > detours.index(c))
        def _():
            detour_copies[c].wait_recv()
            forward_copies[c].start()

    spans = (pl.ds(1, 1), pl.ds(rows, 1), pl.ds(2, rows - 2))
    raw_spans = (pl.ds(0, 1), pl.ds(rows - 1, 1), pl.ds(1, rows - 2))
    raw_layers = [
        [
            vertical(
                side,
                min(j, 2) // 2,
                previous.at[raw, pl.ds((layers - 1, 0)[side], 1), :],
                first.at[span, pl.ds(far_layer[side], 1), body_cols],
            )
            for side in (0, 1)
        ]
        for j, (raw, span) in enumerate(zip(raw_spans, spans))
    ]
    later_layers = [
        [
            vertical(
                side,
                2 + min(j, 2) // 2,
                second.at[span, pl.ds(own_layer[side], 1), body_cols],
                second.at[span, pl.ds(far_layer[side], 1), body_cols],
            )
            for side in (0, 1)
        ]
        for j, span in enumerate(spans)
    ]

    def edge_layers(buffer, slot):
        pair_span = pl.ds(1, 2)
        return [
            vertical(side, slot, *[buffer.at[pair_span, pl.ds(far_layer[side], 1), body_cols]] * 2)
            for side in (0, 1)
        ]

    sum_copies, last_copies = [
        [
            remote(
                src,
                dst.at[k - 1],
                sum_send.at[kind],
                sum_recv.at[kind],
                {"depth": lax.rem(depth + k, depths)},
            )
            for k in range(1, depths)
        ]
        for kind, (src, dst) in enumerate(((sums, others), (last, last_others)))
    ]

    def settle(kind, buffer):
        if depths > 1:
            remote(buffer, buffer, sum_send.at[kind], sum_recv.at[kind], {"depth": depth}).wait()

    def start_layers(group):
        for side in (0, 1):
            pl.when(depth_sends[side])(group[side].start)

    def wait_layers(group):
        for side in (0, 1):
            pl.when(depth_recvs[side])(group[side].wait_recv)

    with jax.named_scope("p02_sends"):
        local_surface.wait()
        for side in (0, 1):
            pl.when(lat_sends[side])(surf_copies[side].start)
        for group in raw_layers[:2]:
            start_layers(group)
        for c in range(RAW[OUTER]):
            send_detour(c)
        for c in range(RAW[PARTNER]):
            partner_copies[c].start()
        for c in range(RAW[OUTER]):
            send_direct(c)
        start_layers(raw_layers[2])

    for copy in [*local_inputs, local_mesh]:
        copy.start()
    zero_tile = jnp.zeros((layers, PAD), jnp.float32)

    def clear_pads(r, carry):
        for buffer in (first, second):
            for start in (0, PAD + columns):
                buffer[r, body_layers, pl.ds(start, PAD)] = zero_tile
        return carry

    lax.fori_loop(1, rows + 1, clear_pads, 0)
    for start in (0, PAD + columns):
        surf[body_rows, pl.ds(start, PAD)] = jnp.zeros((rows, PAD), jnp.float32)
    squares[...] = jnp.zeros_like(squares)

    for side in (0, 1):

        @pl.when(jnp.logical_not(lat_recvs[side]))
        def _(side=side):
            surf[pl.ds(far_row[side], 1), body_cols] = jnp.zeros((1, columns), jnp.float32)
            shift[pl.ds(far_row[side], 1), :] = jnp.zeros((1, columns), jnp.float32)
            first[(0, rows + 1)[side], body_layers, body_cols] = jnp.zeros(
                (layers, columns), jnp.float32
            )
            theirs[OUTER] = jnp.zeros((layers, columns), jnp.float32)

    with jax.named_scope("p04_waitsurf"):
        for copy in local_inputs:
            copy.wait()
        for side in (0, 1):
            pl.when(lat_recvs[side])(surf_copies[side].wait_recv)

    def advect(step, carry):
        c = pl.multiple_of(step * WIDTH, WIDTH)
        cols = pl.ds(c, WIDTH)
        inner = pl.ds(pl.multiple_of(c + PAD, PAD), WIDTH)
        middle, left, right = lanes_beside(surf[body_rows, pl.ds(c, WIDTH + 2 * PAD)], WIDTH)
        before = pltpu.roll(surf[pl.ds(0, rows + TILE), inner], 1, 0)[TILE:]
        after = pltpu.roll(surf[pl.ds(TILE, rows + TILE), inner], rows + TILE - 1, 0)[:rows]
        grad_rows = (after - before) * 0.5
        grad_cols = (right - left) * 0.5
        laplace = after + before + right + left - 4.0 * middle
        names = blocks[:, cols]
        rate = jnp.full(names.shape, rates[0], jnp.float32)
        for label in range(1, blocks_count):
            rate = jnp.where(names == label, rates[label], rate)
        tendency = -vel[0, :, cols] * grad_rows - vel[1, :, cols] * grad_cols + rate * laplace
        fresh = middle + TIME_STEP * flags[:, cols].astype(jnp.float32) * tendency
        new_surface[:, cols] = fresh
        shift[body_rows, cols] = fresh - middle
        return carry

    with jax.named_scope("p05_advect"):
        lax.fori_loop(0, steps, advect, 0)
    with jax.named_scope("p06_sends"):
        send_shift()
        local_mesh.wait()

    def profile_of(index):
        return (total_layers - index).astype(jnp.float32) / total_layers

    base = depth * layers
    profile = profile_of(base + lax.broadcasted_iota(jnp.int32, (layers, PAD), 0))
    above_profile = profile_of(base - 1)
    below_profile = profile_of(base + layers)
    sublane = lax.broadcasted_iota(jnp.int32, (layers, WIDTH), 0)
    at_first = sublane == 0
    at_last = sublane == layers - 1
    above = pl.ds(TILE - 1, 1)
    below = pl.ds(TILE + layers, 1)

    def widen(r, c):
        inner = pl.ds(c + PAD, WIDTH)
        row_shift = jnp.broadcast_to(shift[pl.ds(TILE - 1 + r, 1), pl.ds(c, WIDTH)], (layers, WIDTH))
        wide_profile = jnp.concatenate([profile] * (WIDTH // PAD), axis=1)
        first[r, body_layers, inner] = first[r, body_layers, inner] + row_shift * wide_profile

    def in_plane(source, r, c, top, bottom):
        middle, left, right = lanes_beside(
            source[r, body_layers, pl.ds(c, WIDTH + 2 * PAD)], WIDTH
        )
        upper = jnp.where(at_first, top, pltpu.roll(middle, 1, 0))
        lower = jnp.where(at_last, bottom, pltpu.roll(middle, layers - 1, 0))
        return middle, (left + right) + (upper + lower)

    def first_ends(r, c):
        inner = pl.ds(c + PAD, WIDTH)
        row_shift = shift[pl.ds(TILE - 1 + r, 1), pl.ds(c, WIDTH)]
        top = jnp.where(has_above, first[r, above, inner] + row_shift * above_profile, row_shift)
        bottom = jnp.where(has_below, first[r, below, inner] + row_shift * below_profile, 0.0)
        return top, bottom

    def second_ends(r, c):
        inner = pl.ds(c + PAD, WIDTH)
        row_shift = shift[pl.ds(TILE - 1 + r, 1), pl.ds(c, WIDTH)]
        top = jnp.where(has_above, second[r, above, inner], row_shift)
        bottom = jnp.where(has_below, second[r, below, inner], 0.0)
        return top, bottom

    def weigh(middle, neighbours):
        return (1.0 - RELAX_WEIGHT) * middle + SIDE_WEIGHT * neighbours

    def partial(flow, c):
        inner = pl.ds(c + PAD, WIDTH)
        middle, around = in_plane(first, edges[flow], c, *first_ends(edges[flow], c))
        mine[flow, :, pl.ds(c, WIDTH)] = weigh(
            middle, around + first[inners[flow], body_layers, inner]
        )

    def complete(flow, c):
        inner = pl.ds(c + PAD, WIDTH)
        second[edges[flow], body_layers, inner] = (
            mine[flow, :, pl.ds(c, WIDTH)] + SIDE_WEIGHT * first[halos[flow], body_layers, inner]
        )

    def sweep_once(r, c):
        inner = pl.ds(c + PAD, WIDTH)
        middle, around = in_plane(first, r, c, *first_ends(r, c))
        across = first[r - 1, body_layers, inner] + first[r + 1, body_layers, inner]
        second[r, body_layers, inner] = weigh(middle, across + around)

    def tally(r, c, value):
        field[r - 1, :, pl.ds(c, WIDTH)] = value
        power = value * value
        part = squares[r - 1]
        for top in range(0, layers, TILE):
            for start in range(0, WIDTH, PAD):
                part = part + power[top : top + TILE, start : start + PAD]
        squares[r - 1] = part

    def sweep_twice(r, c):
        inner = pl.ds(c + PAD, WIDTH)
        middle, around = in_plane(second, r, c, *second_ends(r, c))
        across = second[r - 1, body_layers, inner] + second[r + 1, body_layers, inner]
        tally(r, c, weigh(middle, across + around))

    reach = (jnp.float32(SIDE_WEIGHT), jnp.where(has_outer, SIDE_WEIGHT, 0.0))

    def prepare(flow, c):
        inner = pl.ds(c + PAD, WIDTH)
        edge = edges[flow]
        middle, around = in_plane(second, edge, c, *second_ends(edge, c))
        around = around + second[inners[flow], body_layers, inner]
        facing_own = reach[flow] * first[edge, body_layers, inner]
        field[edge - 1, :, pl.ds(c, WIDTH)] = weigh(middle, around + facing_own)

    def finish(flow, c):
        cols = pl.ds(c, WIDTH)
        edge = edges[flow]
        tally(edge, c, field[edge - 1, :, cols] + SIDE_WEIGHT * theirs[flow, :, cols])

    def over(low, count, visit):
        def body(t, carry):
            for step in range(steps):
                visit(t, step * WIDTH)
            return carry

        lax.fori_loop(low, low + count, body, 0)

    with jax.named_scope("p07_widen"):
        over(1, 2, widen)
        over(rows - 1, 2, widen)
        for c in range(RAW[OUTER], CHUNKS):
            send_detour(c)
        for c in range(RAW[PARTNER], CHUNKS):
            partner_copies[c].start()
        for c in range(RAW[OUTER], CHUNKS):
            send_direct(c)
    with jax.named_scope("p08_waitraw"):
        wait_layers(edge_layers(first, 0))
    with jax.named_scope("p09_partial"):
        for flow in (OUTER, PARTNER):
            for step in range(steps):
                partial(flow, step * WIDTH)
    with jax.named_scope("p10_fwd0"):
        forward(0)
    with jax.named_scope("p11_widen"):
        over(3, rows - 4, widen)
        for c in range(CHUNKS, 2 * CHUNKS):
            send_detour(c)
        partner_copies[CHUNKS].start()
    with jax.named_scope("p12_waitraw"):
        wait_layers(raw_layers[2])
    middle_row = rows // 2 + 1
    with jax.named_scope("p13_sweep1"):
        over(2, middle_row - 2, sweep_once)
    with jax.named_scope("p14_fwd1"):
        partner_copies[CHUNKS + 1].start()
        for c in (CHUNKS, CHUNKS + 1):
            send_direct(c)
        forward(1)
    with jax.named_scope("p15_sweep1"):
        over(middle_row, rows - middle_row, sweep_once)
        start_layers(later_layers[2])
    with jax.named_scope("p16_fwd3"):
        for c in range(CHUNKS + 2, 2 * CHUNKS):
            partner_copies[c].start()
            send_direct(c)
        forward(2)
        forward(3)
    with jax.named_scope("p16_fwds"):
        pl.when(has_beyond)(forward_shift)
    with jax.named_scope("p17_waitshift"):
        shift_partner[0].wait_recv()
        pl.when(has_outer)(shift_forward[0].wait_recv)
    for flow in (PARTNER, OUTER):

        def arrive(flow=flow):
            whole_plane(flow).wait_recv()
            for step in range(RAW[flow] * per_piece):
                widen(halos[flow], step * WIDTH)

        with jax.named_scope(f"p18_{flow}{'po'[flow]}"):
            if flow == PARTNER:
                arrive()
            else:
                pl.when(has_outer)(arrive)
            for step in range(steps):
                complete(flow, step * WIDTH)
    with jax.named_scope("p19_edges"):
        for j in (0, 1):
            start_layers(later_layers[j])
    with jax.named_scope("p20_waitlater"):
        wait_layers(later_layers[2])
    with jax.named_scope("p22_sweep2"):
        over(2, middle_row - 2, sweep_twice)
        over(middle_row, rows - middle_row, sweep_twice)
        sums[...] = jnp.sum(squares[...], axis=1)
        for copy in sum_copies:
            copy.start()
    with jax.named_scope("p23_waitlater"):
        forward(CHUNKS)
        forward(CHUNKS + 1)
        wait_layers(edge_layers(second, 2))
    with jax.named_scope("p24_prepare"):
        for flow in (PARTNER, OUTER):
            for step in range(steps):
                prepare(flow, step * WIDTH)
        for c in range(CHUNKS + 2, 2 * CHUNKS):
            forward(c)

    for k in range(CHUNKS):
        with jax.named_scope(f"p25_finish{k}"):
            both = theirs.at[:, :, piece_cols(k)]
            arrivals = remote(
                both, both, plane_send.at[PARTNER], plane_recv.at[2 + k], lat_id(partner)
            )
            pl.when(has_outer)(arrivals.wait_recv)
            pl.when(jnp.logical_not(has_outer))(partner_copies[CHUNKS + k].wait_recv)
            for flow in (PARTNER, OUTER):
                for j in range(per_piece):
                    finish(flow, k * piece + j * WIDTH)

    for flow in (PARTNER, OUTER):
        edge_squares = jnp.sum(squares[edges[flow] - 1], axis=0, keepdims=True)
        last[:, pl.ds(flow * PAD, PAD)] = edge_squares
    for copy in last_copies:
        copy.start()
    settle(0, others)
    total = sums[...]
    for k in range(depths - 1):
        total = total + others[k]
    norm[...] = total
    shift_partner[0].wait_send()
    pl.when(has_outer)(shift_detour[0].wait_send)
    pl.when(has_beyond)(shift_forward[0].wait_send)
    for side in (0, 1):
        pl.when(lat_sends[side])(surf_copies[side].wait_send)
        sent = first.at[pl.ds(1, rows), pl.ds(TILE, 2), body_cols]
        pl.when(depth_sends[side])(vertical(side, 0, sent, sent).wait_send)

    def sent_planes(flow):
        return remote(mine, mine, plane_send.at[flow], plane_recv.at[flow], lat_id(partner))

    sent_planes(PARTNER).wait_send()
    pl.when(has_outer)(sent_planes(OUTER).wait_send)
    for count in range(1, most + 1):
        passed = relay.at[pl.ds(0, count)]
        whole = remote(passed, passed, forward_send.at[0], relay_recv.at[0], lat_id(beyond))
        pl.when(relay_share == count)(whole.wait_send)
    with jax.named_scope("p27_waitsums"):
        settle(1, last_others)
    with jax.named_scope("p28_total"):
        total = last[...]
        for k in range(depths - 1):
            total = total + last_others[k]
        for flow in (PARTNER, OUTER):
            norm[pl.ds(edges[flow] - 1, 1), :] = total[:, flow * PAD : (flow + 1) * PAD]


def deliver(count, surface_in, field_in, total, surface_out, field_out, norm_out, packed, sem):
    copies = [
        pltpu.make_async_copy(field_in, field_out, sem.at[0]),
        pltpu.make_async_copy(surface_in, surface_out, sem.at[1]),
        pltpu.make_async_copy(packed, norm_out, sem.at[2]),
    ]
    for copy in copies[:2]:
        copy.start()
    rows, lanes = total.shape[0], pl.cdiv(total.shape[0], PAD) * PAD
    column = jnp.broadcast_to(jnp.sum(total[...], axis=1, keepdims=True), (rows, lanes))
    ids = lax.broadcasted_iota(jnp.int32, column.shape, 0)
    places = lax.broadcasted_iota(jnp.int32, column.shape, 1)
    flat = jnp.sum(jnp.where(ids == places, column, 0.0), axis=0, keepdims=True)
    packed[...] = jnp.sqrt(flat / count)[0, :rows]
    copies[2].start()
    for copy in copies:
        copy.wait()


def solution(mesh):
    lats, depths = mesh.shape["lat"], mesh.shape["depth"]

    def per_device(surface, velocity, block_map, free_flags, block_rates, previous_mesh):
        rows, layers, columns = previous_mesh.shape
        wide = columns + 2 * PAD
        anywhere = pl.BlockSpec(memory_space=pltpu.HBM)
        f32 = jnp.float32
        others = max(depths - 1, 1)
        most = max((2 * CHUNKS * (lats // 2 - 1)) // (lats // 2), 1)
        dma = pltpu.SemaphoreType.DMA
        held = [
            pltpu.with_memory_space_constraint(value, pltpu.HBM)
            for value in (surface, velocity, block_map, free_flags, block_rates, previous_mesh)
        ]
        results = pl.pallas_call(
            functools.partial(kernel, lats, depths),
            out_shape=(
                pltpu.VMEM(surface.shape, f32),
                pltpu.VMEM(previous_mesh.shape, f32),
                pltpu.VMEM((rows, PAD), f32),
            ),
            in_specs=[anywhere] * 6,
            out_specs=(pl.BlockSpec(memory_space=pltpu.VMEM),) * 3,
            scratch_shapes=[
                pltpu.VMEM((rows + 2 * TILE, wide), f32),
                pltpu.VMEM(velocity.shape, f32),
                pltpu.VMEM(block_map.shape, jnp.int32),
                pltpu.VMEM(free_flags.shape, jnp.int32),
                pltpu.SMEM(block_rates.shape, f32),
                pltpu.VMEM((rows + 2 * TILE, columns), f32),
                pltpu.VMEM((rows + 2, layers + 2 * TILE, wide), f32),
                pltpu.VMEM((rows + 2, layers + 2 * TILE, wide), f32),
                pltpu.VMEM((2, layers, columns), f32),
                pltpu.VMEM((2, layers, columns), f32),
                pltpu.VMEM((most, layers, columns // CHUNKS), f32),
                pltpu.VMEM((1, RAW[OUTER] * (columns // CHUNKS)), f32),
                pltpu.VMEM((rows, TILE, PAD), f32),
                pltpu.VMEM((rows, PAD), f32),
                pltpu.VMEM((others, rows, PAD), f32),
                pltpu.VMEM((1, 2 * PAD), f32),
                pltpu.VMEM((others, 1, 2 * PAD), f32),
                dma((6,)),
                dma((2,)),
                dma((2,)),
                dma((3,)),
                dma((3,)),
                dma((2,)),
                dma((2 + CHUNKS,)),
                dma((most,)),
                dma((1,)),
                dma((2,)),
                dma((2, 4)),
                dma((2,)),
                dma((2,)),
            ],
            compiler_params=pltpu.CompilerParams(
                collective_id=0, has_side_effects=True, vmem_limit_bytes=56 * 1024 * 1024
            ),
            name="advect_and_relax",
        )(*held)
        resident = [pltpu.with_memory_space_constraint(value, pltpu.VMEM) for value in results]
        new_surface, field, norm = pl.pallas_call(
            functools.partial(deliver, layers * depths * columns),
            out_shape=(
                pltpu.HBM(surface.shape, f32),
                pltpu.HBM(previous_mesh.shape, f32),
                pltpu.HBM((rows,), f32),
            ),
            in_specs=[pl.BlockSpec(memory_space=pltpu.VMEM)] * 3,
            out_specs=(anywhere,) * 3,
            scratch_shapes=[pltpu.VMEM((rows,), f32), dma((3,))],
            compiler_params=pltpu.CompilerParams(vmem_limit_bytes=1024 * 1024),
            name="deliver",
        )(*resident)
        return new_surface, field, norm

    return jax.shard_map(
        per_device,
        mesh=mesh,
        in_specs=(
            P("lat", None),
            P(None, "lat", None),
            P("lat", None),
            P("lat", None),
            P(),
            P("lat", "depth", None),
        ),
        out_specs=(P("lat", None), P("lat", "depth", None), P("lat")),
        check_vma=False,
    )
```

```python
import functools

import jax
import jax.numpy as jnp
from jax import lax
from jax.experimental import pallas as pl
from jax.experimental.pallas import tpu as pltpu
from jax.sharding import PartitionSpec as P

ITERS = 2
TIME_STEP = 0.5
RELAX_WEIGHT = 0.8
SIDE_WEIGHT = RELAX_WEIGHT / 6.0
MESH = pl.DeviceIdType.MESH
PAD = 128
TILE = 8
WIDTH = 1024
CHUNKS = 4
RAW = (2, 2)
PARTNER, OUTER = 0, 1


def lanes_beside(window, width):
    span = window.shape[1]
    left = pltpu.roll(window, 1, 1)[:, PAD : PAD + width]
    right = pltpu.roll(window, span - 1, 1)[:, PAD : PAD + width]
    return window[:, PAD : PAD + width], left, right


def kernel(
    lats,
    depths,
    surface,
    velocity,
    block_map,
    free_flags,
    block_rates,
    previous,
    new_surface,
    field,
    norm,
    surf,
    vel,
    blocks,
    flags,
    rates,
    shift,
    first,
    second,
    mine,
    theirs,
    relay,
    relay_shift,
    squares,
    sums,
    others,
    last,
    last_others,
    local_sem,
    near_send,
    near_recv,
    shift_send,
    shift_recv,
    plane_send,
    plane_recv,
    relay_recv,
    forward_send,
    depth_send,
    depth_recv,
    sum_send,
    sum_recv,
):
    rows, layers, columns = previous.shape
    lat = lax.axis_index("lat")
    depth = lax.axis_index("depth")
    total_layers = layers * depths
    blocks_count = block_rates.shape[0]
    steps = columns // WIDTH
    piece = columns // CHUNKS
    per_piece = piece // WIDTH
    has_low, has_high = lat > 0, lat < lats - 1
    has_above, has_below = depth > 0, depth < depths - 1
    body_rows = pl.ds(TILE, rows)
    body_layers = pl.ds(TILE, layers)
    body_cols = pl.ds(PAD, columns)

    odd = lax.rem(lat, 2)
    pair, pairs = lat // 2, lats // 2
    partner = lat + 1 - 2 * odd
    outward = lat - 1 + 2 * odd
    beyond = lat + 2 - 4 * odd
    behind = lat - 2 + 4 * odd
    has_outer = jnp.logical_and(outward >= 0, outward < lats)
    has_beyond = jnp.logical_and(beyond >= 0, beyond < lats)
    down_share = (2 * CHUNKS * pair) // pairs
    up_share = (2 * CHUNKS * (pairs - 1 - pair)) // pairs - lax.rem(depth, 2)
    up_share = jnp.maximum(up_share, 0)
    own_share = jnp.where(odd == 0, down_share, up_share)
    relay_share = jnp.where(odd == 0, up_share, down_share)
    low_side, high_side = odd, 1 - odd
    edges = (1 + (rows - 1) * high_side, 1 + (rows - 1) * low_side)
    inners = (2 + (rows - 3) * high_side, 2 + (rows - 3) * low_side)
    halos = ((rows + 1) * high_side, (rows + 1) * low_side)

    local_surface = pltpu.make_async_copy(
        surface, surf.at[body_rows, body_cols], local_sem.at[0]
    )
    local_inputs = [
        pltpu.make_async_copy(velocity, vel, local_sem.at[1]),
        pltpu.make_async_copy(block_map, blocks, local_sem.at[2]),
        pltpu.make_async_copy(free_flags, flags, local_sem.at[3]),
        pltpu.make_async_copy(block_rates, rates, local_sem.at[5]),
    ]
    local_mesh = pltpu.make_async_copy(
        previous, first.at[pl.ds(1, rows), body_layers, body_cols], local_sem.at[4]
    )

    barrier = pltpu.get_barrier_semaphore()

    def greet(target):
        pl.semaphore_signal(barrier, inc=1, device_id=target, device_id_type=MESH)

    def lat_id(index):
        return {"lat": jnp.clip(index, 0, lats - 1)}

    greet(lat_id(partner))
    pl.when(has_outer)(lambda: greet(lat_id(outward)))
    pl.when(has_beyond)(lambda: greet(lat_id(beyond)))
    pl.when(has_outer)(lambda: greet(lat_id(behind)))
    for k in range(1, depths):
        greet({"depth": lax.rem(depth + k, depths)})
    for copy in [local_surface]:
        copy.start()
    peers = depths + 2 * has_outer.astype(jnp.int32) + has_beyond.astype(jnp.int32)
    with jax.named_scope("p01_barrier"):
        pl.semaphore_wait(barrier, peers)

    def remote(src, dst, send, recv, target):
        return pltpu.make_async_remote_copy(
            src_ref=src,
            dst_ref=dst,
            send_sem=send,
            recv_sem=recv,
            device_id=target,
            device_id_type=MESH,
        )

    def nearby(side, src, dst):
        target = lat_id(lat + 1 if side == 0 else lat - 1)
        return remote(src, dst, near_send.at[side], near_recv.at[side], target)

    def vertical(side, slot, src, dst):
        index = depth + 1 if side == 0 else depth - 1
        target = {"depth": jnp.clip(index, 0, depths - 1)}
        return remote(src, dst, depth_send.at[side], depth_recv.at[side, slot], target)

    def piece_cols(k, pad=0):
        return pl.ds(pad + k * piece, piece)

    lat_sends = (has_high, has_low)
    lat_recvs = (has_low, has_high)
    depth_sends = (has_below, has_above)
    depth_recvs = (has_above, has_below)
    own_layer = (TILE + layers - 1, TILE)
    far_layer = (TILE - 1, TILE + layers)
    own_row = (TILE + rows - 1, TILE)
    far_row = (TILE - 1, TILE + rows)

    surf_copies = [
        nearby(
            side,
            surf.at[pl.ds(own_row[side], 1), body_cols],
            surf.at[pl.ds(far_row[side], 1), body_cols],
        )
        for side in (0, 1)
    ]

    def shift_row(row, flow):
        return shift.at[pl.ds(row, 1), pl.ds(0, RAW[flow] * piece)]

    shift_partner = [
        remote(
            shift_row(own_row[side], PARTNER),
            shift_row(far_row[side], PARTNER),
            shift_send.at[0],
            shift_recv.at[0],
            lat_id(partner),
        )
        for side in (0, 1)
    ]
    shift_detour = [
        remote(
            shift_row(own_row[side], OUTER),
            relay_shift,
            shift_send.at[1],
            shift_recv.at[1],
            lat_id(partner),
        )
        for side in (0, 1)
    ]
    shift_forward = [
        remote(
            relay_shift,
            shift_row(far_row[side], OUTER),
            shift_send.at[2],
            shift_recv.at[2],
            lat_id(beyond),
        )
        for side in (0, 1)
    ]

    def send_shift():
        for side in (0, 1):
            toward = (odd == 0) if side == 0 else (odd == 1)
            away = jnp.logical_and(has_outer, (odd == 1) if side == 0 else (odd == 0))
            pl.when(away)(shift_detour[side].start)
            pl.when(toward)(shift_partner[side].start)

    def forward_shift():
        shift_detour[0].wait_recv()
        for side in (0, 1):
            pl.when((odd == 0) if side == 0 else (odd == 1))(shift_forward[side].start)

    def source(flow, c):
        if c < RAW[flow]:
            return previous.at[edges[flow] - 1, :, piece_cols(c)]
        if c < CHUNKS:
            return first.at[edges[flow], body_layers, piece_cols(c, PAD)]
        return mine.at[flow, :, piece_cols(c - CHUNKS)]

    def landing(flow, halo, c):
        if c < CHUNKS:
            return first.at[halo, body_layers, piece_cols(c, PAD)]
        return theirs.at[flow, :, piece_cols(c - CHUNKS)]

    partner_halo = (rows + 1) * low_side
    outward_halo = (rows + 1) * high_side
    beyond_halo = (rows + 1) * low_side
    pieces = range(2 * CHUNKS)
    order = list(pieces)
    most = (2 * CHUNKS * (pairs - 1)) // pairs
    detours = order[:most]

    def landed(flow, c):
        return plane_recv.at[flow if c < CHUNKS else 2 + c - CHUNKS]

    partner_copies = [
        remote(
            source(PARTNER, c),
            landing(PARTNER, partner_halo, c),
            plane_send.at[PARTNER],
            landed(PARTNER, c),
            lat_id(partner),
        )
        for c in pieces
    ]
    outward_copies = [
        remote(
            source(OUTER, c),
            landing(OUTER, outward_halo, c),
            plane_send.at[OUTER],
            landed(OUTER, c),
            lat_id(outward),
        )
        for c in pieces
    ]
    detour_copies = {
        c: remote(
            source(OUTER, c),
            relay.at[slot],
            plane_send.at[OUTER],
            relay_recv.at[slot],
            lat_id(partner),
        )
        for slot, c in enumerate(detours)
    }
    forward_copies = {
        c: remote(
            relay.at[slot],
            landing(OUTER, beyond_halo, c),
            forward_send.at[0],
            landed(OUTER, c),
            lat_id(beyond),
        )
        for slot, c in enumerate(detours)
    }

    def whole_plane(flow):
        whole = first.at[halos[flow], body_layers, body_cols]
        return remote(whole, whole, plane_send.at[flow], plane_recv.at[flow], lat_id(partner))

    def send_detour(c):
        if c in detour_copies:
            pl.when(own_share > detours.index(c))(detour_copies[c].start)

    def send_direct(c):
        direct = has_outer
        if c in detour_copies:
            direct = jnp.logical_and(has_outer, own_share <= detours.index(c))
        pl.when(direct)(outward_copies[c].start)

    def forward(c):
        if c not in forward_copies:
            return

        @pl.when(relay_share > detours.index(c))
        def _():
            detour_copies[c].wait_recv()
            forward_copies[c].start()

    spans = (pl.ds(1, 1), pl.ds(rows, 1), pl.ds(2, rows - 2))
    raw_spans = (pl.ds(0, 1), pl.ds(rows - 1, 1), pl.ds(1, rows - 2))
    raw_layers = [
        [
            vertical(
                side,
                min(j, 2) // 2,
                previous.at[raw, pl.ds((layers - 1, 0)[side], 1), :],
                first.at[span, pl.ds(far_layer[side], 1), body_cols],
            )
            for side in (0, 1)
        ]
        for j, (raw, span) in enumerate(zip(raw_spans, spans))
    ]
    later_layers = [
        [
            vertical(
                side,
                2 + min(j, 2) // 2,
                second.at[span, pl.ds(own_layer[side], 1), body_cols],
                second.at[span, pl.ds(far_layer[side], 1), body_cols],
            )
            for side in (0, 1)
        ]
        for j, span in enumerate(spans)
    ]

    def edge_layers(buffer, slot):
        pair_span = pl.ds(1, 2)
        return [
            vertical(side, slot, *[buffer.at[pair_span, pl.ds(far_layer[side], 1), body_cols]] * 2)
            for side in (0, 1)
        ]

    sum_copies, last_copies = [
        [
            remote(
                src,
                dst.at[k - 1],
                sum_send.at[kind],
                sum_recv.at[kind],
                {"depth": lax.rem(depth + k, depths)},
            )
            for k in range(1, depths)
        ]
        for kind, (src, dst) in enumerate(((sums, others), (last, last_others)))
    ]

    def settle(kind, buffer):
        if depths > 1:
            remote(buffer, buffer, sum_send.at[kind], sum_recv.at[kind], {"depth": depth}).wait()

    def start_layers(group):
        for side in (0, 1):
            pl.when(depth_sends[side])(group[side].start)

    def wait_layers(group):
        for side in (0, 1):
            pl.when(depth_recvs[side])(group[side].wait_recv)

    with jax.named_scope("p02_sends"):
        local_surface.wait()
        for side in (0, 1):
            pl.when(lat_sends[side])(surf_copies[side].start)
        for c in range(RAW[OUTER]):
            send_detour(c)
        for c in range(RAW[PARTNER]):
            partner_copies[c].start()
        for group in raw_layers[:2]:
            start_layers(group)
        for c in range(RAW[OUTER]):
            send_direct(c)
        start_layers(raw_layers[2])

    for copy in [*local_inputs, local_mesh]:
        copy.start()
    zero_tile = jnp.zeros((layers, PAD), jnp.float32)

    def clear_pads(r, carry):
        for buffer in (first, second):
            for start in (0, PAD + columns):
                buffer[r, body_layers, pl.ds(start, PAD)] = zero_tile
        return carry

    lax.fori_loop(1, rows + 1, clear_pads, 0)
    for start in (0, PAD + columns):
        surf[body_rows, pl.ds(start, PAD)] = jnp.zeros((rows, PAD), jnp.float32)
    squares[...] = jnp.zeros_like(squares)

    for side in (0, 1):

        @pl.when(jnp.logical_not(lat_recvs[side]))
        def _(side=side):
            surf[pl.ds(far_row[side], 1), body_cols] = jnp.zeros((1, columns), jnp.float32)
            shift[pl.ds(far_row[side], 1), :] = jnp.zeros((1, columns), jnp.float32)
            first[(0, rows + 1)[side], body_layers, body_cols] = jnp.zeros(
                (layers, columns), jnp.float32
            )
            theirs[OUTER] = jnp.zeros((layers, columns), jnp.float32)

    with jax.named_scope("p04_waitsurf"):
        for copy in local_inputs:
            copy.wait()
        for side in (0, 1):
            pl.when(lat_recvs[side])(surf_copies[side].wait_recv)

    def advect(step, carry):
        c = pl.multiple_of(step * WIDTH, WIDTH)
        cols = pl.ds(c, WIDTH)
        inner = pl.ds(pl.multiple_of(c + PAD, PAD), WIDTH)
        middle, left, right = lanes_beside(surf[body_rows, pl.ds(c, WIDTH + 2 * PAD)], WIDTH)
        before = pltpu.roll(surf[pl.ds(0, rows + TILE), inner], 1, 0)[TILE:]
        after = pltpu.roll(surf[pl.ds(TILE, rows + TILE), inner], rows + TILE - 1, 0)[:rows]
        grad_rows = (after - before) * 0.5
        grad_cols = (right - left) * 0.5
        laplace = after + before + right + left - 4.0 * middle
        names = blocks[:, cols]
        rate = jnp.full(names.shape, rates[0], jnp.float32)
        for label in range(1, blocks_count):
            rate = jnp.where(names == label, rates[label], rate)
        tendency = -vel[0, :, cols] * grad_rows - vel[1, :, cols] * grad_cols + rate * laplace
        fresh = middle + TIME_STEP * flags[:, cols].astype(jnp.float32) * tendency
        new_surface[:, cols] = fresh
        shift[body_rows, cols] = fresh - middle
        return carry

    with jax.named_scope("p05_advect"):
        lax.fori_loop(0, steps, advect, 0)
    with jax.named_scope("p06_sends"):
        send_shift()
        local_mesh.wait()

    def profile_of(index):
        return (total_layers - index).astype(jnp.float32) / total_layers

    base = depth * layers
    profile = profile_of(base + lax.broadcasted_iota(jnp.int32, (layers, PAD), 0))
    above_profile = profile_of(base - 1)
    below_profile = profile_of(base + layers)
    sublane = lax.broadcasted_iota(jnp.int32, (layers, WIDTH), 0)
    at_first = sublane == 0
    at_last = sublane == layers - 1
    above = pl.ds(TILE - 1, 1)
    below = pl.ds(TILE + layers, 1)

    def widen(r, c):
        inner = pl.ds(c + PAD, WIDTH)
        row_shift = jnp.broadcast_to(shift[pl.ds(TILE - 1 + r, 1), pl.ds(c, WIDTH)], (layers, WIDTH))
        wide_profile = jnp.concatenate([profile] * (WIDTH // PAD), axis=1)
        first[r, body_layers, inner] = first[r, body_layers, inner] + row_shift * wide_profile

    def in_plane(source, r, c, top, bottom):
        middle, left, right = lanes_beside(
            source[r, body_layers, pl.ds(c, WIDTH + 2 * PAD)], WIDTH
        )
        upper = jnp.where(at_first, top, pltpu.roll(middle, 1, 0))
        lower = jnp.where(at_last, bottom, pltpu.roll(middle, layers - 1, 0))
        return middle, (left + right) + (upper + lower)

    def first_ends(r, c):
        inner = pl.ds(c + PAD, WIDTH)
        row_shift = shift[pl.ds(TILE - 1 + r, 1), pl.ds(c, WIDTH)]
        top = jnp.where(has_above, first[r, above, inner] + row_shift * above_profile, row_shift)
        bottom = jnp.where(has_below, first[r, below, inner] + row_shift * below_profile, 0.0)
        return top, bottom

    def second_ends(r, c):
        inner = pl.ds(c + PAD, WIDTH)
        row_shift = shift[pl.ds(TILE - 1 + r, 1), pl.ds(c, WIDTH)]
        top = jnp.where(has_above, second[r, above, inner], row_shift)
        bottom = jnp.where(has_below, second[r, below, inner], 0.0)
        return top, bottom

    def weigh(middle, neighbours):
        return (1.0 - RELAX_WEIGHT) * middle + SIDE_WEIGHT * neighbours

    def partial(flow, c):
        inner = pl.ds(c + PAD, WIDTH)
        middle, around = in_plane(first, edges[flow], c, *first_ends(edges[flow], c))
        mine[flow, :, pl.ds(c, WIDTH)] = weigh(
            middle, around + first[inners[flow], body_layers, inner]
        )

    def complete(flow, c):
        inner = pl.ds(c + PAD, WIDTH)
        second[edges[flow], body_layers, inner] = (
            mine[flow, :, pl.ds(c, WIDTH)] + SIDE_WEIGHT * first[halos[flow], body_layers, inner]
        )

    def sweep_once(r, c):
        inner = pl.ds(c + PAD, WIDTH)
        middle, around = in_plane(first, r, c, *first_ends(r, c))
        across = first[r - 1, body_layers, inner] + first[r + 1, body_layers, inner]
        second[r, body_layers, inner] = weigh(middle, across + around)

    def tally(r, c, value):
        field[r - 1, :, pl.ds(c, WIDTH)] = value
        power = value * value
        part = squares[r - 1]
        for top in range(0, layers, TILE):
            for start in range(0, WIDTH, PAD):
                part = part + power[top : top + TILE, start : start + PAD]
        squares[r - 1] = part

    def sweep_twice(r, c):
        inner = pl.ds(c + PAD, WIDTH)
        middle, around = in_plane(second, r, c, *second_ends(r, c))
        across = second[r - 1, body_layers, inner] + second[r + 1, body_layers, inner]
        tally(r, c, weigh(middle, across + around))

    reach = (jnp.float32(SIDE_WEIGHT), jnp.where(has_outer, SIDE_WEIGHT, 0.0))

    def prepare(flow, c):
        inner = pl.ds(c + PAD, WIDTH)
        edge = edges[flow]
        middle, around = in_plane(second, edge, c, *second_ends(edge, c))
        around = around + second[inners[flow], body_layers, inner]
        facing_own = reach[flow] * first[edge, body_layers, inner]
        field[edge - 1, :, pl.ds(c, WIDTH)] = weigh(middle, around + facing_own)

    def finish(flow, c):
        cols = pl.ds(c, WIDTH)
        edge = edges[flow]
        tally(edge, c, field[edge - 1, :, cols] + SIDE_WEIGHT * theirs[flow, :, cols])

    def over(low, count, visit):
        def body(t, carry):
            for step in range(steps):
                visit(t, step * WIDTH)
            return carry

        lax.fori_loop(low, low + count, body, 0)

    with jax.named_scope("p07_widen"):
        over(1, 2, widen)
        over(rows - 1, 2, widen)
        for c in range(RAW[OUTER], CHUNKS):
            send_detour(c)
        for c in range(RAW[PARTNER], CHUNKS):
            partner_copies[c].start()
        for c in range(RAW[OUTER], CHUNKS):
            send_direct(c)
    with jax.named_scope("p08_waitraw"):
        wait_layers(edge_layers(first, 0))
    with jax.named_scope("p09_partial"):
        for flow in (OUTER, PARTNER):
            for step in range(steps):
                partial(flow, step * WIDTH)
    with jax.named_scope("p10_fwd0"):
        forward(0)
    with jax.named_scope("p11_widen"):
        over(3, rows - 4, widen)
        for c in range(CHUNKS, 2 * CHUNKS):
            send_detour(c)
        partner_copies[CHUNKS].start()
    with jax.named_scope("p12_waitraw"):
        wait_layers(raw_layers[2])
    middle_row = rows // 2 + 1
    with jax.named_scope("p13_sweep1"):
        over(2, middle_row - 2, sweep_once)
    with jax.named_scope("p14_fwd1"):
        partner_copies[CHUNKS + 1].start()
        for c in (CHUNKS, CHUNKS + 1):
            send_direct(c)
        forward(1)
    with jax.named_scope("p15_sweep1"):
        over(middle_row, rows - middle_row, sweep_once)
        start_layers(later_layers[2])
    with jax.named_scope("p16_fwd3"):
        for c in range(CHUNKS + 2, 2 * CHUNKS):
            partner_copies[c].start()
            send_direct(c)
        forward(2)
        forward(3)
    with jax.named_scope("p16_fwds"):
        pl.when(has_beyond)(forward_shift)
    with jax.named_scope("p17_waitshift"):
        shift_partner[0].wait_recv()
        pl.when(has_outer)(shift_forward[0].wait_recv)
    for flow in (PARTNER, OUTER):

        def arrive(flow=flow):
            whole_plane(flow).wait_recv()
            for step in range(RAW[flow] * per_piece):
                widen(halos[flow], step * WIDTH)

        with jax.named_scope(f"p18_{flow}{'po'[flow]}"):
            if flow == PARTNER:
                arrive()
            else:
                pl.when(has_outer)(arrive)
            for step in range(steps):
                complete(flow, step * WIDTH)
    with jax.named_scope("p19_edges"):
        for j in (0, 1):
            start_layers(later_layers[j])
    with jax.named_scope("p20_waitlater"):
        wait_layers(later_layers[2])
    with jax.named_scope("p22_sweep2"):
        over(2, middle_row - 2, sweep_twice)
        over(middle_row, rows - middle_row, sweep_twice)
        sums[...] = jnp.sum(squares[...], axis=1)
        for copy in sum_copies:
            copy.start()
    with jax.named_scope("p23_waitlater"):
        forward(CHUNKS)
        forward(CHUNKS + 1)
        wait_layers(edge_layers(second, 2))
    with jax.named_scope("p24_prepare"):
        for flow in (PARTNER, OUTER):
            for step in range(steps):
                prepare(flow, step * WIDTH)
        for c in range(CHUNKS + 2, 2 * CHUNKS):
            forward(c)

    for k in range(CHUNKS):
        with jax.named_scope(f"p25_finish{k}"):
            both = theirs.at[:, :, piece_cols(k)]
            arrivals = remote(
                both, both, plane_send.at[PARTNER], plane_recv.at[2 + k], lat_id(partner)
            )
            pl.when(has_outer)(arrivals.wait_recv)
            pl.when(jnp.logical_not(has_outer))(partner_copies[CHUNKS + k].wait_recv)
            for flow in (PARTNER, OUTER):
                for j in range(per_piece):
                    finish(flow, k * piece + j * WIDTH)

    for flow in (PARTNER, OUTER):
        edge_squares = jnp.sum(squares[edges[flow] - 1], axis=0, keepdims=True)
        last[:, pl.ds(flow * PAD, PAD)] = edge_squares
    for copy in last_copies:
        copy.start()
    settle(0, others)
    total = sums[...]
    for k in range(depths - 1):
        total = total + others[k]
    norm[...] = total
    shift_partner[0].wait_send()
    pl.when(has_outer)(shift_detour[0].wait_send)
    pl.when(has_beyond)(shift_forward[0].wait_send)
    for side in (0, 1):
        pl.when(lat_sends[side])(surf_copies[side].wait_send)
        sent = first.at[pl.ds(1, rows), pl.ds(TILE, 2), body_cols]
        pl.when(depth_sends[side])(vertical(side, 0, sent, sent).wait_send)

    def sent_planes(flow):
        return remote(mine, mine, plane_send.at[flow], plane_recv.at[flow], lat_id(partner))

    sent_planes(PARTNER).wait_send()
    pl.when(has_outer)(sent_planes(OUTER).wait_send)
    for count in range(1, most + 1):
        passed = relay.at[pl.ds(0, count)]
        whole = remote(passed, passed, forward_send.at[0], relay_recv.at[0], lat_id(beyond))
        pl.when(relay_share == count)(whole.wait_send)
    with jax.named_scope("p27_waitsums"):
        settle(1, last_others)
    with jax.named_scope("p28_total"):
        total = last[...]
        for k in range(depths - 1):
            total = total + last_others[k]
        for flow in (PARTNER, OUTER):
            norm[pl.ds(edges[flow] - 1, 1), :] = total[:, flow * PAD : (flow + 1) * PAD]


def deliver(count, surface_in, field_in, total, surface_out, field_out, norm_out, packed, sem):
    copies = [
        pltpu.make_async_copy(field_in, field_out, sem.at[0]),
        pltpu.make_async_copy(surface_in, surface_out, sem.at[1]),
        pltpu.make_async_copy(packed, norm_out, sem.at[2]),
    ]
    for copy in copies[:2]:
        copy.start()
    rows, lanes = total.shape[0], pl.cdiv(total.shape[0], PAD) * PAD
    column = jnp.broadcast_to(jnp.sum(total[...], axis=1, keepdims=True), (rows, lanes))
    ids = lax.broadcasted_iota(jnp.int32, column.shape, 0)
    places = lax.broadcasted_iota(jnp.int32, column.shape, 1)
    flat = jnp.sum(jnp.where(ids == places, column, 0.0), axis=0, keepdims=True)
    packed[...] = jnp.sqrt(flat / count)[0, :rows]
    copies[2].start()
    for copy in copies:
        copy.wait()


def solution(mesh):
    lats, depths = mesh.shape["lat"], mesh.shape["depth"]

    def per_device(surface, velocity, block_map, free_flags, block_rates, previous_mesh):
        rows, layers, columns = previous_mesh.shape
        wide = columns + 2 * PAD
        anywhere = pl.BlockSpec(memory_space=pltpu.HBM)
        f32 = jnp.float32
        others = max(depths - 1, 1)
        most = max((2 * CHUNKS * (lats // 2 - 1)) // (lats // 2), 1)
        dma = pltpu.SemaphoreType.DMA
        held = [
            pltpu.with_memory_space_constraint(value, pltpu.HBM)
            for value in (surface, velocity, block_map, free_flags, block_rates, previous_mesh)
        ]
        results = pl.pallas_call(
            functools.partial(kernel, lats, depths),
            out_shape=(
                pltpu.VMEM(surface.shape, f32),
                pltpu.VMEM(previous_mesh.shape, f32),
                pltpu.VMEM((rows, PAD), f32),
            ),
            in_specs=[anywhere] * 6,
            out_specs=(pl.BlockSpec(memory_space=pltpu.VMEM),) * 3,
            scratch_shapes=[
                pltpu.VMEM((rows + 2 * TILE, wide), f32),
                pltpu.VMEM(velocity.shape, f32),
                pltpu.VMEM(block_map.shape, jnp.int32),
                pltpu.VMEM(free_flags.shape, jnp.int32),
                pltpu.SMEM(block_rates.shape, f32),
                pltpu.VMEM((rows + 2 * TILE, columns), f32),
                pltpu.VMEM((rows + 2, layers + 2 * TILE, wide), f32),
                pltpu.VMEM((rows + 2, layers + 2 * TILE, wide), f32),
                pltpu.VMEM((2, layers, columns), f32),
                pltpu.VMEM((2, layers, columns), f32),
                pltpu.VMEM((most, layers, columns // CHUNKS), f32),
                pltpu.VMEM((1, RAW[OUTER] * (columns // CHUNKS)), f32),
                pltpu.VMEM((rows, TILE, PAD), f32),
                pltpu.VMEM((rows, PAD), f32),
                pltpu.VMEM((others, rows, PAD), f32),
                pltpu.VMEM((1, 2 * PAD), f32),
                pltpu.VMEM((others, 1, 2 * PAD), f32),
                dma((6,)),
                dma((2,)),
                dma((2,)),
                dma((3,)),
                dma((3,)),
                dma((2,)),
                dma((2 + CHUNKS,)),
                dma((most,)),
                dma((1,)),
                dma((2,)),
                dma((2, 4)),
                dma((2,)),
                dma((2,)),
            ],
            compiler_params=pltpu.CompilerParams(
                collective_id=0, has_side_effects=True, vmem_limit_bytes=56 * 1024 * 1024
            ),
            name="advect_and_relax",
        )(*held)
        resident = [pltpu.with_memory_space_constraint(value, pltpu.VMEM) for value in results]
        new_surface, field, norm = pl.pallas_call(
            functools.partial(deliver, layers * depths * columns),
            out_shape=(
                pltpu.HBM(surface.shape, f32),
                pltpu.HBM(previous_mesh.shape, f32),
                pltpu.HBM((rows,), f32),
            ),
            in_specs=[pl.BlockSpec(memory_space=pltpu.VMEM)] * 3,
            out_specs=(anywhere,) * 3,
            scratch_shapes=[pltpu.VMEM((rows,), f32), dma((3,))],
            compiler_params=pltpu.CompilerParams(vmem_limit_bytes=1024 * 1024),
            name="deliver",
        )(*resident)
        return new_surface, field, norm

    return jax.shard_map(
        per_device,
        mesh=mesh,
        in_specs=(
            P("lat", None),
            P(None, "lat", None),
            P("lat", None),
            P("lat", None),
            P(),
            P("lat", "depth", None),
        ),
        out_specs=(P("lat", None), P("lat", "depth", None), P("lat")),
        check_vma=False,
    )
```
